32 devices in a mesh: seq: 8 (over z, x), grp: 4 (over y, core).
Axes of the slice: x: 2, y: 2, z: 4, core: 2. Of those that a mesh axis runs over, the one named last changes fastest.
Arguments:
- delta_codes: int32 [16, 16, 2048, 128], P('grp', None, 'seq'), may hold values from -63 to 63, as said below
- scale_index: int32 [16, 16, 128], P('grp', None, 'seq'), may hold values from 0 to 15
- anchor_codes: int32 [16, 16, 128], P('grp'), may hold values from -8 to 7
- scale_table: float32 [16, 128], replicated, may hold values from 5e-05 to 0.0005
- anchor_scale: float32 [128], replicated, may hold values from 0.0001 to 0.001
Outputs:
- decode_cache: bfloat16 [4, 64, 2048, 128], P('grp', 'seq')
The draws below stay inside these ranges and needn't reach their ends.
Inputs may be any that keep to these rules, and one draw needn't show every extreme that they name: `delta_codes`: for every sequence, head and channel, the running sum of the codes from the sequence's first token lies in -32 .. 31 after every token, and in -2 .. 1 after the last token of each group of 16 tokens.
All inputs are finite; a program needn't handle non-finite values.
Results may differ from the reference program's by a relative error of at most 0.001.
Values may be sent and summed in bfloat16 or wider, within the bound.
A program may use at most 128 MiB of HBM per device.

```python
import math
import jax
import jax.numpy as jnp
from jax import lax

HEAD_DIM = 128
KV_HEADS = 16
GROUP_LEN = 16
LEVELS = 16
SEQS = 16
LENGTH = 2048
N_GRP = 4


def draw_delta_codes(key, part):
    running_key = jax.random.fold_in(key, 11)
    running = jax.random.randint(running_key, (SEQS, KV_HEADS, LENGTH, HEAD_DIM), -32, 32, dtype=jnp.int32)
    position = lax.broadcasted_iota(jnp.int32, (1, 1, LENGTH, 1), 2)
    group_end = position % GROUP_LEN == GROUP_LEN - 1
    running = jnp.where(group_end, jnp.remainder(running, 4) - 2, running)
    earlier = jnp.pad(running[:, :, :-1, :], ((0, 0), (0, 0), (1, 0), (0, 0)))
    return running - earlier


def plant(values, key, low, largest):
    dims = values.shape
    place = [jax.random.randint(jax.random.fold_in(key, axis), (), 0, dims[axis]) for axis in range(len(dims))]
    values = values.at[tuple(place)].set(low)
    longest = dims.index(max(dims))
    place[longest] = (place[longest] + 1) % dims[longest]
    return values.at[tuple(place)].set(largest)


def setup_inputs(seed: int = 0) -> dict:
    seeds = jax.random.split(jax.random.key(seed), 6)
    delta_codes = draw_delta_codes(jax.random.fold_in(seeds[5], 71), 0)
    scale_index = plant(jax.random.randint(seeds[1], (SEQS, KV_HEADS, LENGTH // GROUP_LEN), 0, LEVELS), jax.random.fold_in(seeds[1], 1), 0, LEVELS - 1).astype(jnp.int32)
    anchor_codes = plant(jax.random.randint(seeds[2], (SEQS, KV_HEADS, HEAD_DIM), -8, 8), jax.random.fold_in(seeds[2], 1), -8, 7).astype(jnp.int32)
    scale_table = jnp.clip(jnp.exp(jax.random.uniform(seeds[3], (LEVELS, HEAD_DIM), jnp.float32, math.log(4.999999873689376e-05), math.log(0.0005))), 4.999999873689376e-05, 0.0005)
    anchor_scale = jnp.clip(jnp.exp(jax.random.uniform(seeds[4], (HEAD_DIM,), jnp.float32, math.log(0.0001), math.log(0.001))), 0.0001, 0.001)
    return {"delta_codes": delta_codes, "scale_index": scale_index, "anchor_codes": anchor_codes, "scale_table": scale_table, "anchor_scale": anchor_scale}


def reference(delta_codes, scale_index, anchor_codes, scale_table, anchor_scale):
    def one_sequence(items):
        code_vals, scale_ids, anchors = items
        scales = scale_table[scale_ids]
        shaped = code_vals.astype(jnp.float32).reshape(KV_HEADS, LENGTH // GROUP_LEN, GROUP_LEN, HEAD_DIM)
        deltas = shaped * scales[:, :, None, :]
        summed = jnp.cumsum(deltas.reshape(KV_HEADS, LENGTH, HEAD_DIM), axis=1)
        anchor_vals = anchors.astype(jnp.float32) * anchor_scale
        return (summed + anchor_vals[:, None, :]).astype(jnp.bfloat16)

    rebuilt = lax.map(one_sequence, (delta_codes, scale_index, anchor_codes))
    arranged = rebuilt.reshape(SEQS, N_GRP, KV_HEADS // N_GRP, LENGTH, HEAD_DIM).transpose(1, 0, 2, 3, 4)
    return arranged.reshape(N_GRP, SEQS * (KV_HEADS // N_GRP), LENGTH, HEAD_DIM)
```

```python
import functools

import jax
import jax.numpy as jnp
from jax import lax
from jax.experimental import pallas as pl
from jax.experimental.pallas import tpu as pltpu
from jax.sharding import PartitionSpec as P

MESH = pl.DeviceIdType.MESH
CHUNKS = 4
LAG = 1
HIGHEST = lax.Precision.HIGHEST


def exchange(
    codes, index_hbm, anchor_hbm, table_hbm, anchor_scale_hbm,
    landed, scales_ref, base_ref,
    raw, sums, relay, index_out, index_in, anchor_out, anchor_in,
    load_sem, send_sem, recv_sem, isend_sem, irecv_sem, asend_sem, arecv_sem,
    relay_sem, forward_sem,
    index_ref, anchor_ref, table_ref, anchor_scale_ref, small_sem,
):
    seqs, grps = lax.axis_size("seq"), lax.axis_size("grp")
    s, g = lax.axis_index("seq"), lax.axis_index("grp")
    blocks, rows, tokens, channels = sums.shape
    heads = codes.shape[1] // grps
    per_grp = blocks // grps
    half = grps // 2
    partner = lax.rem(g + half, grps)
    chunks = relay.shape[1]
    chunk_rows = rows // chunks
    passed = blocks // 2 * chunks
    seq_rows, head_rows = max(1, rows // heads), min(rows, heads)
    levels = table_ref.shape[0]
    groups = index_hbm.shape[2]
    group_len = tokens // groups

    def place_from(d, own):
        e = d // 2
        side = lax.rem(own // half + 1 + d, 2)
        h = side * half + lax.rem(own + e // per_grp, half)
        i = lax.rem(s + e, per_grp)
        first = i * rows
        return h, own * per_grp + i, first // heads, h * heads + lax.rem(first, heads)

    def place(d):
        return place_from(d, g)

    def is_me(d):
        h, to_s, _, _ = place(d)
        return jnp.logical_and(h == g, to_s == s)

    def load(d):
        _, _, b0, k0 = place(d)
        return pltpu.make_async_copy(
            codes.at[pl.ds(b0, seq_rows), pl.ds(k0, head_rows)], raw.at[d], load_sem.at[d]
        )

    def remote(src, dst, ssem, rsem, d):
        h, to_s, _, _ = place(d)
        return pltpu.make_async_remote_copy(
            src_ref=src, dst_ref=dst, send_sem=ssem, recv_sem=rsem,
            device_id={"seq": to_s, "grp": h}, device_id_type=MESH,
        )

    def window(j):
        return landed.at[:, pl.ds(pl.multiple_of(j * tokens, tokens), tokens), :]

    def send_sums(d):
        return remote(sums.at[d], window(s), send_sem.at[d], recv_sem.at[s], d)

    def at_partner(d):
        h, to_s, _, _ = place(d)
        return jnp.logical_and(h == partner, to_s == s)

    def part(c):
        return pl.ds(c * chunk_rows, chunk_rows)

    def send_relay(e, c):
        return pltpu.make_async_remote_copy(
            src_ref=sums.at[2 * e, part(c)], dst_ref=relay.at[e, c],
            send_sem=send_sem.at[2 * e], recv_sem=relay_sem.at[e, c],
            device_id={"seq": s, "grp": partner}, device_id_type=MESH,
        )

    def send_part(d, c):
        span = pl.ds(pl.multiple_of(s * tokens, tokens), tokens)
        return remote(
            sums.at[d, part(c)], landed.at[part(c), span, :], send_sem.at[d], recv_sem.at[s], d
        )

    def relayed(e):
        h, to_s, _, _ = place_from(2 * e, partner)
        return jnp.logical_not(jnp.logical_and(h == g, to_s == s))

    def forward(e, c):
        h, to_s, _, _ = place_from(2 * e, partner)
        span = pl.ds(pl.multiple_of(s * tokens, tokens), tokens)
        return pltpu.make_async_remote_copy(
            src_ref=relay.at[e, c], dst_ref=landed.at[pl.ds(c * chunk_rows, chunk_rows), span, :],
            send_sem=forward_sem.at[e], recv_sem=recv_sem.at[s],
            device_id={"seq": to_s, "grp": h}, device_id_type=MESH,
        )

    def pass_on(n):
        e, c = n // chunks, lax.rem(n, chunks)

        @pl.when(relayed(e))
        def _():
            send_relay(e, c).wait_recv()
            forward(e, c).start()

    def send_index(d):
        return remote(index_out.at[d], index_in.at[s], isend_sem.at[d], irecv_sem.at[s], d)

    def send_anchor(d):
        return remote(anchor_out.at[d], anchor_in, asend_sem.at[d], arecv_sem, d)

    ahead = min(2, blocks)
    for d in range(ahead):
        load(d).start()

    small = (
        (index_hbm, index_ref), (anchor_hbm, anchor_ref),
        (table_hbm, table_ref), (anchor_scale_hbm, anchor_scale_ref),
    )
    fetches = [
        pltpu.make_async_copy(src, dst, small_sem.at[n]) for n, (src, dst) in enumerate(small)
    ]
    for fetch in fetches:
        fetch.start()

    barrier = pltpu.get_barrier_semaphore()
    from_g = s // per_grp

    inside = lax.rem(from_g, half) == lax.rem(g, half)

    @pl.loop(0, 2 * seqs)
    def _(n):
        j = n // 2
        to_g = lax.rem(from_g + lax.rem(n, 2) * half, grps)

        @pl.when(jnp.logical_not(jnp.logical_and(j == s, to_g == g)))
        def _():
            pl.semaphore_signal(
                barrier, inc=1, device_id={"seq": j, "grp": to_g}, device_id_type=MESH
            )

    @pl.when(jnp.logical_not(inside))
    def _():
        pl.semaphore_signal(
            barrier, inc=1, device_id={"seq": s, "grp": partner}, device_id_type=MESH
        )

    expected = 2 * blocks + jnp.where(inside, -1, 1)

    t_out = lax.broadcasted_iota(jnp.int32, (tokens, tokens), 0)
    t_in = lax.broadcasted_iota(jnp.int32, (tokens, tokens), 1)
    same = t_out // group_len == t_in // group_len
    within = jnp.where(jnp.logical_and(same, t_out >= t_in), 1.0, 0.0).astype(jnp.bfloat16)

    @pl.loop(0, blocks)
    def _(d):
        load(d).wait()

        @pl.when(d + ahead < blocks)
        def _():
            load(d + ahead).start()

        away = jnp.logical_not(is_me(d))
        via = jnp.logical_and(lax.rem(d, 2) == 0, jnp.logical_not(at_partner(d)))
        straight = jnp.logical_and(away, jnp.logical_not(via))
        for c in range(chunks):
            for r in range(c * chunk_rows, (c + 1) * chunk_rows):
                x = raw[d, r // head_rows, r % head_rows].astype(jnp.float32).astype(jnp.bfloat16)
                run = jnp.dot(within, x, preferred_element_type=jnp.float32)
                sums[d, r] = run.astype(jnp.bfloat16)

            if c == 0:
                @pl.when(d == 0)
                def _():
                    pl.semaphore_wait(barrier, expected)

            @pl.when(via)
            def _():
                send_relay(d // 2, c).start()

            @pl.when(straight)
            def _():
                send_part(d, c).start()

        @pl.when(jnp.logical_and(d >= LAG, d - LAG < passed))
        def _():
            pass_on(d - LAG)

    for fetch in fetches:
        fetch.wait()

    @pl.loop(0, blocks)
    def _(d):
        _, _, b0, k0 = place(d)
        for b in range(seq_rows):
            these = pl.ds(b * head_rows, head_rows)
            index_out[d, these, :] = index_ref[b0 + b, pl.ds(k0, head_rows), :]
            anchor_out[d, these, :] = anchor_ref[b0 + b, pl.ds(k0, head_rows), :]

        @pl.when(jnp.logical_not(is_me(d)))
        def _():
            send_index(d).start()

            @pl.when(s == 0)
            def _():
                send_anchor(d).start()

    @pl.loop(min(blocks - LAG, passed), passed)
    def _(n):
        pass_on(n)

    @pl.loop(0, blocks)
    def _(d):
        @pl.when(is_me(d))
        def _():
            index_in[s] = index_out[d]
            for r in range(rows):
                landed[r, pl.ds(pl.multiple_of(s * tokens, tokens), tokens), :] = sums[d, r]

            @pl.when(s == 0)
            def _():
                anchor_in[...] = anchor_out[d]

    mine = jnp.logical_and(from_g == g, s == 0)

    @pl.when(jnp.logical_not(mine))
    def _():
        send_anchor(0).wait_recv()

    for r in range(rows):
        base_ref[r] = anchor_in[pl.ds(r, 1), :].astype(jnp.float32) * anchor_scale_ref[...]

    def from_me(j):
        return jnp.logical_and(j == s, from_g == g)

    @pl.loop(0, seqs)
    def _(j):
        @pl.when(jnp.logical_not(from_me(j)))
        def _():
            remote(index_out.at[0], index_in.at[j], isend_sem.at[0], irecv_sem.at[j], 0).wait_recv()

        table = table_ref[...]
        for r in range(rows):
            ids = jnp.broadcast_to(index_in[j, pl.ds(r, 1), :], (levels, groups))
            hot = (ids == lax.broadcasted_iota(jnp.int32, (levels, groups), 0)).astype(jnp.float32)
            found = lax.dot_general(
                hot, table, (((0,), (0,)), ((), ())),
                precision=HIGHEST, preferred_element_type=jnp.float32,
            )
            scales_ref[r, pl.ds(pl.multiple_of(j * groups, groups), groups), :] = found

    @pl.loop(0, seqs)
    def _(j):
        @pl.when(jnp.logical_not(from_me(j)))
        def _():
            remote(sums.at[0], window(j), send_sem.at[0], recv_sem.at[j], 0).wait_recv()

    @pl.loop(0, blocks)
    def _(d):
        @pl.when(jnp.logical_not(is_me(d)))
        def _():
            send_index(d).wait_send()

            @pl.when(s == 0)
            def _():
                send_anchor(d).wait_send()

            send_sums(d).wait_send()

    @pl.loop(0, blocks // 2)
    def _(e):
        @pl.when(relayed(e))
        def _():
            for c in range(chunks):
                forward(e, c).wait_send()


def rebuild(sums_ref, scales_ref, base_ref, out_hbm, built, out_sem):
    many, length, channels = built.shape
    groups = scales_ref.shape[1]
    group_len = length // groups
    stores = [pltpu.make_async_copy(built.at[r], out_hbm.at[0, r], out_sem.at[r]) for r in range(many)]
    for r in range(many):

        def step(j, base, r=r):
            at = pl.multiple_of(j * group_len, group_len)
            x = sums_ref[r, pl.ds(at, group_len), :].astype(jnp.float32)
            grown = x * scales_ref[r, pl.ds(j, 1), :]
            built[r, pl.ds(at, group_len), :] = (grown + base).astype(jnp.bfloat16)
            return base + grown[group_len - 1:]

        lax.fori_loop(0, groups, step, base_ref[r], unroll=16)
        stores[r].start()
    for copy in stores:
        copy.wait()


def on_device(delta_codes, scale_index, anchor_codes, scale_table, anchor_scale):
    seqs, grps = lax.axis_size("seq"), lax.axis_size("grp")
    seq_local, kv_heads, tokens, channels = delta_codes.shape
    groups = scale_index.shape[2]
    heads = kv_heads // grps
    rows = seq_local * grps * heads // seqs
    blocks = seq_local * kv_heads // rows
    seq_rows, head_rows = max(1, rows // heads), min(rows, heads)
    chunks = min(rows, CHUNKS)
    length = seqs * tokens
    vmem = pl.BlockSpec(memory_space=pltpu.VMEM)
    hbm = pl.BlockSpec(memory_space=pltpu.HBM)
    sums, scales, base = pl.pallas_call(
        exchange,
        out_shape=(
            jax.ShapeDtypeStruct((rows, length, channels), jnp.bfloat16),
            jax.ShapeDtypeStruct((rows, seqs * groups, channels), jnp.float32),
            jax.ShapeDtypeStruct((rows, 1, channels), jnp.float32),
        ),
        in_specs=[hbm] * 5,
        out_specs=(vmem, vmem, vmem),
        scratch_shapes=[
            pltpu.VMEM((blocks, seq_rows, head_rows, tokens, channels), jnp.int32),
            pltpu.VMEM((blocks, rows, tokens, channels), jnp.bfloat16),
            pltpu.VMEM((blocks // 2, chunks, rows // chunks, tokens, channels), jnp.bfloat16),
            pltpu.VMEM((blocks, rows, groups), jnp.int32),
            pltpu.VMEM((seqs, rows, groups), jnp.int32),
            pltpu.VMEM((blocks, rows, channels), jnp.int32),
            pltpu.VMEM((rows, channels), jnp.int32),
            pltpu.SemaphoreType.DMA((blocks,)),
            pltpu.SemaphoreType.DMA((blocks,)),
            pltpu.SemaphoreType.DMA((seqs,)),
            pltpu.SemaphoreType.DMA((blocks,)),
            pltpu.SemaphoreType.DMA((seqs,)),
            pltpu.SemaphoreType.DMA((blocks,)),
            pltpu.SemaphoreType.DMA,
            pltpu.SemaphoreType.DMA((blocks // 2, chunks)),
            pltpu.SemaphoreType.DMA((blocks // 2,)),
            pltpu.VMEM(scale_index.shape, jnp.int32),
            pltpu.VMEM(anchor_codes.shape, jnp.int32),
            pltpu.VMEM(scale_table.shape, jnp.float32),
            pltpu.VMEM((1, channels), jnp.float32),
            pltpu.SemaphoreType.DMA((4,)),
        ],
        compiler_params=pltpu.CompilerParams(
            collective_id=0, has_side_effects=True, vmem_limit_bytes=48 * 1024 * 1024
        ),
        name="exchange",
    )(*(pltpu.with_memory_space_constraint(a, pltpu.HBM) for a in (delta_codes, scale_index, anchor_codes, scale_table, anchor_scale[None])))

    out = pl.pallas_call(
        rebuild,
        out_shape=jax.ShapeDtypeStruct((1, rows, length, channels), jnp.bfloat16),
        in_specs=[vmem] * 3,
        out_specs=hbm,
        scratch_shapes=[
            pltpu.VMEM(sums.shape, jnp.bfloat16),
            pltpu.SemaphoreType.DMA((rows,)),
        ],
        compiler_params=pltpu.CompilerParams(vmem_limit_bytes=16 * 1024 * 1024),
        name="rebuild",
    )(sums, scales, base)
    return out


def solution(mesh):
    placed = (P("grp", None, "seq", None), P("grp", None, "seq"), P("grp", None, None), P(), P())
    return jax.shard_map(
        on_device,
        mesh=mesh,
        in_specs=placed,
        out_specs=P("grp", "seq", None, None),
        check_vma=False,
    )
```

```python
import jax
import jax.numpy as jnp
from jax import lax
from jax.experimental import pallas as pl
from jax.experimental.pallas import tpu as pltpu
from jax.sharding import PartitionSpec as P

MESH = pl.DeviceIdType.MESH
MOVED = (1,)
SMALL = 6
LEAD = 0
LAG = 4
KEEP = 1
HIGHEST = lax.Precision.HIGHEST


def grow(landed, scales_ref, base_ref, r):
    groups = scales_ref.shape[1]
    group_len = landed.shape[1] // groups

    def step(j, base):
        at = pl.multiple_of(j * group_len, group_len)
        x = landed[r, pl.ds(at, group_len), :].astype(jnp.float32)
        grown = x * scales_ref[r, pl.ds(j, 1), :]
        return at, (grown + base).astype(jnp.bfloat16), base + grown[group_len - 1:]

    return groups, step


def exchange(
    codes, index_hbm, anchor_hbm, table_hbm, anchor_scale_hbm,
    landed, scales_ref, base_ref,
    raw, sums, relay, index_out, index_hold, index_in, anchor_out, anchor_in,
    first_sem, load_sem, send_sem, recv_sem, ihold_sem, irecv_sem, arecv_sem,
    relay_half_sem, relay_sem,
    index_ref, anchor_ref, table_ref, anchor_scale_ref, small_sem, wide_ref,
):
    seqs, grps = lax.axis_size("seq"), lax.axis_size("grp")
    s, g = lax.axis_index("seq"), lax.axis_index("grp")
    blocks, rows, tokens, channels = sums.shape
    heads = codes.shape[1] // grps
    per_grp = blocks // grps
    half = grps // 2
    partner = lax.rem(g + half, grps)
    seq_rows, head_rows = raw.shape[0], raw.shape[2]
    levels = table_ref.shape[0]
    groups = index_hbm.shape[2]
    group_len = tokens // groups
    piece = tokens // 2
    zone = s // per_grp
    zone_partner = lax.rem(zone + half, grps)
    via = zone != g
    pass_on = zone != partner
    mine = zone == g
    also = jnp.logical_and
    chunks = rows + 1

    def place_from(d, own):
        side, e, i = lax.rem(d, 2), lax.rem(d // 2, half), d // 2 // half
        h = lax.rem(own // half + 1 + side, 2) * half + lax.rem(own + e, half)
        first = i * rows
        return h, own * per_grp + i, first // heads, h * heads + lax.rem(first, heads)

    def is_me(d):
        h, to_s, _, _ = place_from(d, g)
        return also(h == g, to_s == s)

    def load(d, b, sem):
        _, _, b0, k0 = place_from(d, g)
        return pltpu.make_async_copy(codes.at[b0 + b, pl.ds(k0, head_rows)], raw.at[b, d], sem)

    def loaded(b, i):
        skip = 1 if b == 0 and i == 0 else 0
        these = raw.at[b, pl.ds(i * 2 * half + skip, 2 * half - skip)]
        return pltpu.make_async_copy(these, these, load_sem.at[b, i])

    def spot(r, lo, size):
        return landed.at[r, pl.ds(pl.multiple_of(s * tokens + lo, size), size), :]

    def remote(src, dst, rsem, h, to_s):
        return pltpu.make_async_remote_copy(
            src_ref=src, dst_ref=dst, send_sem=send_sem, recv_sem=rsem,
            device_id={"seq": to_s, "grp": h}, device_id_type=MESH,
        )

    def here(ref, rsem):
        return remote(ref, ref, rsem, g, s)

    def relay_sem_at(d, r, lo, size):
        if size == tokens:
            return relay_sem.at[d // 2 // half, r - 1]
        return relay_half_sem.at[d // 2, lo // piece]

    def send_relay(d, r, lo, size):
        return remote(
            sums.at[d, r, pl.ds(lo, size)], relay.at[d // 2, r, pl.ds(lo, size)],
            relay_sem_at(d, r, lo, size), partner, s,
        )

    def send_part(d, r, lo, size):
        h, to_s, _, _ = place_from(d, g)
        return remote(sums.at[d, r, pl.ds(lo, size)], spot(r, lo, size), recv_sem.at[r], h, to_s)

    def forward(d, r, lo, size):
        h, to_s, _, _ = place_from(d, partner)
        return remote(
            relay.at[d // 2, r, pl.ds(lo, size)], spot(r, lo, size), recv_sem.at[r], h, to_s
        )

    def send_index(d):
        h, to_s, _, _ = place_from(d, g)
        return remote(index_out.at[d], index_in.at[s], irecv_sem, h, to_s)

    def hold_index(d):
        return remote(index_out.at[d], index_hold.at[d // 2], ihold_sem, partner, s)

    def forward_index(d):
        h, to_s, _, _ = place_from(d, partner)
        return remote(index_hold.at[d // 2], index_in.at[s], irecv_sem, h, to_s)

    def send_anchor(d):
        h, to_s, _, _ = place_from(d, g)
        return remote(anchor_out.at[d], anchor_in, arecv_sem, h, to_s)

    def sends_anchor(d):
        _, to_s, _, _ = place_from(d, g)
        return also(to_s == s, jnp.logical_not(is_me(d)))

    load(0, 0, first_sem).start()
    barrier = pltpu.get_barrier_semaphore()

    @pl.loop(0, seqs)
    def _(j):
        straight = jnp.logical_or(zone // half == g // half, j // per_grp == zone)
        to_g = jnp.where(straight, zone, zone_partner)

        @pl.when(jnp.logical_not(also(j == s, to_g == g)))
        def _():
            pl.semaphore_signal(
                barrier, inc=1, device_id={"seq": j, "grp": to_g}, device_id_type=MESH
            )

    @pl.when(pass_on)
    def _():
        pl.semaphore_signal(
            barrier, inc=1, device_id={"seq": s, "grp": partner}, device_id_type=MESH
        )

    @pl.when(also(g == zone_partner, lax.rem(s, per_grp) == 0))
    def _():
        @pl.loop(0, seqs if MOVED else 0)
        def _(j):
            @pl.when(j // per_grp != zone)
            def _():
                pl.semaphore_signal(
                    barrier, inc=1, device_id={"seq": j, "grp": zone}, device_id_type=MESH
                )

    expected = (
        blocks // 2
        + jnp.where(via, 1 + (1 if MOVED else 0), blocks // 2 - 1)
        + jnp.where(pass_on, blocks // 2, 0)
    )

    for b in range(seq_rows):
        @pl.loop(1 if b == 0 else 0, blocks)
        def _(d, b=b):
            load(d, b, load_sem.at[b, d // (2 * half)]).start()

    small = (
        (index_hbm, index_ref), (anchor_hbm, anchor_ref),
        (table_hbm, table_ref), (anchor_scale_hbm, anchor_scale_ref),
    )
    fetches = [
        pltpu.make_async_copy(src, dst, small_sem.at[n]) for n, (src, dst) in enumerate(small)
    ]
    for fetch in fetches:
        fetch.start()

    t_out = lax.broadcasted_iota(jnp.int32, (tokens, tokens), 0)
    t_in = lax.broadcasted_iota(jnp.int32, (tokens, tokens), 1)
    same = t_out // group_len == t_in // group_len
    within = jnp.where(also(same, t_out >= t_in), 1.0, 0.0).astype(jnp.bfloat16)

    def compute(d, r, lo, size):
        x = raw[r // head_rows, d, lax.rem(r, head_rows), pl.ds(lo, size), :]
        x = x.astype(jnp.float32).astype(jnp.bfloat16)
        run = jnp.dot(within[:size, :size], x, preferred_element_type=jnp.float32)
        sums[d, r, pl.ds(lo, size), :] = run.astype(jnp.bfloat16)

    def is_moved(e, i, lo, size):
        hit = size == piece and e == 0 and lo // piece in MOVED
        return i == 0 if hit else i < 0

    def send_all(i, r, lo, size):
        for e in range(half):
            d = (i * half + e) * 2
            if e == 0 and size == piece and lo == 0:
                @pl.when(i > 0)
                def _():
                    compute(d, r, lo, size)
            else:
                compute(d, r, lo, size)

            relayed = also(via, jnp.logical_not(is_moved(e, i, lo, size)))

            @pl.when(relayed)
            def _(d=d):
                send_relay(d, r, lo, size).start()

            @pl.when(jnp.logical_not(relayed))
            def _(d=d):
                send_part(d, r, lo, size).start()

        for e in range(half):
            d = (i * half + e) * 2 + 1
            compute(d, r, lo, size)

            @pl.when(jnp.logical_not(is_me(d)))
            def _(d=d):
                send_part(d, r, lo, size).start()

    def forward_all(i, r, lo, size):
        def from_relay(e):
            d = (i * half + e) * 2
            forward(d, r, lo, size).start()

        if size == tokens:
            both = relay.at[pl.ds(i * half, half), r]
            here(both, relay_sem.at[i, r - 1]).wait_recv()
            for e in range(half):
                from_relay(e)
        else:
            for e in range(half):
                @pl.when(jnp.logical_not(is_moved(e, i, lo, size)))
                def _(e=e):
                    send_relay((i * half + e) * 2, r, lo, size).wait_recv()
                    from_relay(e)

    lane = lax.broadcasted_iota(jnp.int32, (groups, rows * groups), 1)
    spread = (lax.rem(lane, groups) == lax.broadcasted_iota(jnp.int32, lane.shape, 0))
    lane = lax.broadcasted_iota(jnp.int32, (rows, rows * groups), 1)
    own_row = lane // groups == lax.broadcasted_iota(jnp.int32, lane.shape, 0)

    def send_small():
        for fetch in fetches:
            fetch.wait()

        ids = index_ref[...].astype(jnp.float32).astype(jnp.bfloat16)
        ids = ids.reshape(-1, groups)
        wide = jnp.dot(ids, spread.astype(jnp.bfloat16), preferred_element_type=jnp.float32)
        wide_ref[...] = wide.reshape(wide_ref.shape)

        @pl.loop(0, blocks)
        def _(d):
            _, _, b0, k0 = place_from(d, g)
            line = 0.0
            for b in range(seq_rows):
                these = pl.ds(b * head_rows, head_rows)
                anchor_out[d, these, :] = anchor_ref[b0 + b, pl.ds(k0, head_rows), :]
                kept = jnp.where(own_row[b * head_rows:(b + 1) * head_rows],
                                 wide_ref[b0 + b, pl.ds(k0, head_rows), :], 0.0)
                line += jnp.sum(kept, axis=0, keepdims=True)
            index_out[d] = line.astype(jnp.int32)

            relayed = also(lax.rem(d, 2) == 0, via)

            @pl.when(relayed)
            def _():
                hold_index(d).start()

            @pl.when(jnp.logical_not(jnp.logical_or(relayed, is_me(d))))
            def _():
                send_index(d).start()

            @pl.when(sends_anchor(d))
            def _():
                send_anchor(d).start()

    steps = (chunks + LEAD * (per_grp - 1)) * per_grp
    pltpu.make_async_copy(raw.at[0, 0], raw.at[0, 0], first_sem).wait()
    compute(0, 0, 0, piece)
    pl.semaphore_wait(barrier, expected)

    def at_chunk(n, ready, do):
        i = lax.rem(n, per_grp)
        c = n // per_grp - LEAD * i
        for lo in (0, piece):
            @pl.when(also(ready, c == lo // piece))
            def _(lo=lo):
                do(i, 0, lo, piece)

        @pl.when(also(ready, also(c >= 2, c < chunks)))
        def _():
            do(i, c - 1, 0, tokens)

    def wait_and_send(i, r, lo, size):
        if lo == 0:
            for b in range(seq_rows):
                for k in range(per_grp):
                    @pl.when(also(i == k, r == b * head_rows))
                    def _(b=b, k=k):
                        loaded(b, k).wait()
        send_all(i, r, lo, size)

    @pl.loop(0, steps + LAG)
    def _(n):
        at_chunk(jnp.maximum(n - LAG, 0), also(n >= LAG, pass_on), forward_all)
        at_chunk(n, n < steps, wait_and_send)

        @pl.when(n == SMALL)
        def _():
            send_small()

        @pl.when(also(pass_on, n == SMALL + LAG))
        def _():
            here(index_hold, ihold_sem).wait_recv()

            @pl.loop(0, blocks // 2)
            def _(e):
                forward_index(e * 2).start()

    @pl.loop(0, blocks)
    def _(d):
        @pl.when(is_me(d))
        def _():
            index_in[s] = index_out[d]
            anchor_in[...] = anchor_out[d]
            for r in range(rows):
                landed[r, pl.ds(pl.multiple_of(s * tokens, tokens), tokens), :] = sums[d, r]

    def fewer(ref, sem, axis):
        def part(count):
            at = [slice(None)] * (axis + 1)
            at[axis] = pl.ds(0, count)
            return ref.at[tuple(at)]

        size = ref.shape[axis]

        @pl.when(mine)
        def _():
            here(part(size - size // seqs), sem).wait_recv()

        @pl.when(jnp.logical_not(mine))
        def _():
            here(ref, sem).wait_recv()

    @pl.when(jnp.logical_not(mine))
    def _():
        here(anchor_in, arecv_sem).wait_recv()

    for r in range(rows):
        base_ref[r] = anchor_in[pl.ds(r, 1), :].astype(jnp.float32) * anchor_scale_ref[...]

    fewer(index_in, irecv_sem, 0)

    @pl.loop(0, seqs)
    def _(j):
        many = rows * groups
        ids = jnp.broadcast_to(index_in[j], (levels, many))
        hot = (ids == lax.broadcasted_iota(jnp.int32, (levels, many), 0)).astype(jnp.float32)
        found = lax.dot_general(
            hot, table_ref[...], (((0,), (0,)), ((), ())),
            precision=HIGHEST, preferred_element_type=jnp.float32,
        )
        for r in range(rows):
            scales_ref[r, pl.ds(pl.multiple_of(j * groups, groups), groups), :] = (
                found[r * groups:(r + 1) * groups]
            )

    @pl.loop(0, rows)
    def _(r):
        fewer(landed.at[r], recv_sem.at[r], 0)

        @pl.when(r < rows - min(KEEP, rows))
        def _():
            many, step = grow(landed, scales_ref, base_ref, r)

            def put(j, base):
                at, built, base = step(j, base)
                landed[r, pl.ds(at, group_len), :] = built
                return base

            lax.fori_loop(0, many, put, base_ref[r], unroll=16)

    def sent(ref):
        here(ref, recv_sem.at[0]).wait_send()

    @pl.when(mine)
    def _():
        sent(sums.at[pl.ds(0, blocks - 1)])
        sent(index_out.at[pl.ds(0, blocks - 1)])
        for _ in range(grps - 1):
            sent(anchor_out.at[0])

    @pl.when(jnp.logical_not(mine))
    def _():
        sent(sums)
        sent(index_out)

    @pl.when(pass_on)
    def _():
        sent(index_hold)
        if MOVED:
            sent(relay.at[pl.ds(1, blocks // 2 - 1)])
            if rows > 1:
                sent(relay.at[0, pl.ds(1, rows - 1)])
            for _ in range(2 - len(MOVED)):
                sent(relay.at[0, 0, pl.ds(0, piece)])
        else:
            sent(relay)


def rebuild(landed, scales_ref, base_ref, out_hbm, built, out_sem):
    rows = landed.shape[0]
    keep = built.shape[0]
    done = rows - keep
    stores = []
    if done:
        stores.append(pltpu.make_async_copy(
            landed.at[pl.ds(0, done)], out_hbm.at[0, pl.ds(0, done)], out_sem.at[keep]
        ))
        stores[0].start()
    for q in range(keep):
        r = done + q
        many, step = grow(landed, scales_ref, base_ref, r)
        group_len = landed.shape[1] // many

        def put(j, base, q=q, step=step):
            at, grown, base = step(j, base)
            built[q, pl.ds(at, group_len), :] = grown
            return base

        lax.fori_loop(0, many, put, base_ref[r], unroll=16)
        stores.append(pltpu.make_async_copy(built.at[q], out_hbm.at[0, r], out_sem.at[q]))
        stores[-1].start()
    for store in stores:
        store.wait()


def on_device(delta_codes, scale_index, anchor_codes, scale_table, anchor_scale):
    seqs, grps = lax.axis_size("seq"), lax.axis_size("grp")
    seq_local, kv_heads, tokens, channels = delta_codes.shape
    groups = scale_index.shape[2]
    heads = kv_heads // grps
    rows = seq_local * grps * heads // seqs
    blocks = seq_local * kv_heads // rows
    seq_rows, head_rows = max(1, rows // heads), min(rows, heads)
    keep = min(KEEP, rows)
    length = seqs * tokens
    vmem = pl.BlockSpec(memory_space=pltpu.VMEM)
    hbm = pl.BlockSpec(memory_space=pltpu.HBM)
    operands = (delta_codes, scale_index, anchor_codes, scale_table, anchor_scale[None])
    landed, scales, base = pl.pallas_call(
        exchange,
        out_shape=(
            jax.ShapeDtypeStruct((rows, length, channels), jnp.bfloat16),
            jax.ShapeDtypeStruct((rows, seqs * groups, channels), jnp.float32),
            jax.ShapeDtypeStruct((rows, 1, channels), jnp.float32),
        ),
        in_specs=[hbm] * 5,
        out_specs=(vmem, vmem, vmem),
        scratch_shapes=[
            pltpu.VMEM((seq_rows, blocks, head_rows, tokens, channels), jnp.int32),
            pltpu.VMEM((blocks, rows, tokens, channels), jnp.bfloat16),
            pltpu.VMEM((blocks // 2, rows, tokens, channels), jnp.bfloat16),
            pltpu.VMEM((blocks, 1, rows * groups), jnp.int32),
            pltpu.VMEM((blocks // 2, 1, rows * groups), jnp.int32),
            pltpu.VMEM((seqs, 1, rows * groups), jnp.int32),
            pltpu.VMEM((blocks, rows, channels), jnp.int32),
            pltpu.VMEM((rows, channels), jnp.int32),
            pltpu.SemaphoreType.DMA,
            pltpu.SemaphoreType.DMA((seq_rows, blocks // grps)),
            pltpu.SemaphoreType.DMA,
            pltpu.SemaphoreType.DMA((rows,)),
            pltpu.SemaphoreType.DMA,
            pltpu.SemaphoreType.DMA,
            pltpu.SemaphoreType.DMA,
            pltpu.SemaphoreType.DMA((blocks // 2, 2)),
            pltpu.SemaphoreType.DMA((blocks // grps, max(1, rows - 1))),
            pltpu.VMEM(scale_index.shape, jnp.int32),
            pltpu.VMEM(anchor_codes.shape, jnp.int32),
            pltpu.VMEM(scale_table.shape, jnp.float32),
            pltpu.VMEM((1, channels), jnp.float32),
            pltpu.SemaphoreType.DMA((4,)),
            pltpu.VMEM(scale_index.shape[:2] + (rows * groups,), jnp.float32),
        ],
        compiler_params=pltpu.CompilerParams(
            collective_id=0, has_side_effects=True, vmem_limit_bytes=48 * 1024 * 1024
        ),
        name="exchange",
    )(*(pltpu.with_memory_space_constraint(x, pltpu.HBM) for x in operands))

    return pl.pallas_call(
        rebuild,
        out_shape=jax.ShapeDtypeStruct((1, rows, length, channels), jnp.bfloat16),
        in_specs=[vmem] * 3,
        out_specs=hbm,
        scratch_shapes=[
            pltpu.VMEM((keep, length, channels), jnp.bfloat16),
            pltpu.SemaphoreType.DMA((keep + 1,)),
        ],
        compiler_params=pltpu.CompilerParams(vmem_limit_bytes=16 * 1024 * 1024),
        name="rebuild",
    )(landed, scales, base)


def solution(mesh):
    placed = (P("grp", None, "seq", None), P("grp", None, "seq"), P("grp", None, None), P(), P())
    return jax.shard_map(
        on_device,
        mesh=mesh,
        in_specs=placed,
        out_specs=P("grp", "seq", None, None),
        check_vma=False,
    )
```

```python
import jax
import jax.numpy as jnp
from jax import lax
from jax.experimental import pallas as pl
from jax.experimental.pallas import tpu as pltpu
from jax.sharding import PartitionSpec as P

MESH = pl.DeviceIdType.MESH
MOVED = (1,)
SMALL = 6
LEAD = 0
LAG = 4
RELAY_LAG = 1
KEEP = 1
HIGHEST = lax.Precision.HIGHEST


def grow(landed, scales_ref, base_ref, r):
    groups = scales_ref.shape[1]
    group_len = landed.shape[1] // groups

    def step(j, base):
        at = pl.multiple_of(j * group_len, group_len)
        x = landed[r, pl.ds(at, group_len), :].astype(jnp.float32)
        grown = x * scales_ref[r, pl.ds(j, 1), :]
        return at, (grown + base).astype(jnp.bfloat16), base + grown[group_len - 1:]

    return groups, step


def arrival_cuts(rows):
    return sorted({0, rows // 2, rows - min(KEEP, rows), rows})


def exchange(
    codes, index_hbm, anchor_hbm, table_hbm, anchor_scale_hbm,
    landed, scales_ref, base_ref,
    raw, sums, relay, index_out, index_hold, index_in, anchor_out, anchor_in,
    first_sem, rest_sem, load_sem, send_sem, recv_sem, ihold_sem, irecv_sem, arecv_sem,
    relay_half_sem, relay_sem,
    index_ref, anchor_ref, table_ref, anchor_scale_ref, small_sem, wide_ref,
):
    seqs, grps = lax.axis_size("seq"), lax.axis_size("grp")
    s, g = lax.axis_index("seq"), lax.axis_index("grp")
    blocks, rows, tokens, channels = sums.shape
    heads = codes.shape[1] // grps
    per_grp = blocks // grps
    half = grps // 2
    partner = lax.rem(g + half, grps)
    seq_rows, head_rows = raw.shape[0], raw.shape[2]
    levels = table_ref.shape[0]
    groups = index_hbm.shape[2]
    group_len = tokens // groups
    piece = tokens // 2
    zone = s // per_grp
    zone_partner = lax.rem(zone + half, grps)
    via = zone != g
    pass_on = zone != partner
    mine = zone == g
    also = jnp.logical_and
    chunks = rows + 1
    cuts = arrival_cuts(rows)

    def arrival_sem(r):
        group = 0
        for at in cuts[1:-1]:
            group = group + jnp.where(r >= at, 1, 0)
        return recv_sem.at[group]


    def place_from(d, own):
        side, e, i = lax.rem(d, 2), lax.rem(d // 2, half), d // 2 // half
        h = lax.rem(own // half + 1 + side, 2) * half + lax.rem(e + i, half)
        first = i * rows
        return h, own * per_grp + i, first // heads, h * heads + lax.rem(first, heads)

    def is_me(d):
        h, to_s, _, _ = place_from(d, g)
        return also(h == g, to_s == s)

    def load(d, b, sem):
        _, _, b0, k0 = place_from(d, g)
        return pltpu.make_async_copy(codes.at[b0 + b, pl.ds(k0, head_rows)], raw.at[b, d], sem)

    def loaded(b, i):
        these = raw.at[b, pl.ds(i * 2 * half, 2 * half)]
        return pltpu.make_async_copy(these, these, load_sem.at[b, i])

    def spot(r, lo, size):
        return landed.at[r, pl.ds(pl.multiple_of(s * tokens + lo, size), size), :]

    def remote(src, dst, rsem, h, to_s):
        return pltpu.make_async_remote_copy(
            src_ref=src, dst_ref=dst, send_sem=send_sem, recv_sem=rsem,
            device_id={"seq": to_s, "grp": h}, device_id_type=MESH,
        )

    def here(ref, rsem):
        return remote(ref, ref, rsem, g, s)

    def relay_sem_at(d, r, lo, size):
        if size == tokens:
            return relay_sem.at[d // 2 // half, r - 1]
        return relay_half_sem.at[d // 2, lo // piece]

    def send_relay(d, r, lo, size):
        return remote(
            sums.at[d, r, pl.ds(lo, size)], relay.at[d // 2, r, pl.ds(lo, size)],
            relay_sem_at(d, r, lo, size), partner, s,
        )

    def send_part(d, r, lo, size):
        h, to_s, _, _ = place_from(d, g)
        return remote(sums.at[d, r, pl.ds(lo, size)], spot(r, lo, size), arrival_sem(r), h, to_s)

    def forward(d, r, lo, size):
        h, to_s, _, _ = place_from(d, partner)
        return remote(
            relay.at[d // 2, r, pl.ds(lo, size)], spot(r, lo, size), arrival_sem(r), h, to_s
        )

    def send_index(d):
        h, to_s, _, _ = place_from(d, g)
        return remote(index_out.at[d], index_in.at[s], irecv_sem, h, to_s)

    def hold_index(d):
        return remote(index_out.at[d], index_hold.at[d // 2], ihold_sem, partner, s)

    def forward_index(d):
        h, to_s, _, _ = place_from(d, partner)
        return remote(index_hold.at[d // 2], index_in.at[s], irecv_sem, h, to_s)

    def send_anchor(d):
        h, to_s, _, _ = place_from(d, g)
        return remote(anchor_out.at[d], anchor_in, arecv_sem, h, to_s)

    def sends_anchor(d):
        _, to_s, _, _ = place_from(d, g)
        return also(to_s == s, jnp.logical_not(is_me(d)))

    ahead = 2 * half

    def first_rows(d, lo, size, sem):
        _, _, b0, k0 = place_from(d, g)
        return pltpu.make_async_copy(
            codes.at[b0, pl.ds(k0 + lo, size)], raw.at[0, d, pl.ds(lo, size)], sem
        )

    def first_loaded(lo, size, sem):
        these = raw.at[0, pl.ds(0, ahead), pl.ds(lo, size)]
        return pltpu.make_async_copy(these, these, sem)

    for d in range(ahead):
        first_rows(d, 0, 1, first_sem).start()

    barrier = pltpu.get_barrier_semaphore()

    @pl.loop(0, seqs)
    def _(j):
        straight = jnp.logical_or(zone // half == g // half, j // per_grp == zone)
        to_g = jnp.where(straight, zone, zone_partner)

        @pl.when(jnp.logical_not(also(j == s, to_g == g)))
        def _():
            pl.semaphore_signal(
                barrier, inc=1, device_id={"seq": j, "grp": to_g}, device_id_type=MESH
            )

    @pl.when(pass_on)
    def _():
        pl.semaphore_signal(
            barrier, inc=1, device_id={"seq": s, "grp": partner}, device_id_type=MESH
        )

    gets_moved = also(g // half == zone_partner // half, lax.rem(g, half) == 0)

    @pl.when(also(gets_moved, lax.rem(s, per_grp) == 0))
    def _():
        @pl.loop(0, seqs if MOVED else 0)
        def _(j):
            @pl.when(j // per_grp != zone)
            def _():
                pl.semaphore_signal(
                    barrier, inc=1, device_id={"seq": j, "grp": zone}, device_id_type=MESH
                )

    expected = (
        blocks // 2
        + jnp.where(via, 1 + (1 if MOVED else 0), blocks // 2 - 1)
        + jnp.where(pass_on, blocks // 2, 0)
    )

    if head_rows > 1:
        for d in range(ahead):
            first_rows(d, 1, head_rows - 1, rest_sem).start()

    for b in range(seq_rows):
        @pl.loop(ahead if b == 0 else 0, blocks)
        def _(d, b=b):
            load(d, b, load_sem.at[b, d // (2 * half)]).start()

    fetch_index = pltpu.make_async_copy(index_hbm, index_ref, small_sem.at[0])
    fetch_anchor = pltpu.make_async_copy(anchor_hbm, anchor_ref, small_sem.at[1])
    fetch_index.start()
    fetch_anchor.start()

    t_out = lax.broadcasted_iota(jnp.int32, (tokens, tokens), 0)
    t_in = lax.broadcasted_iota(jnp.int32, (tokens, tokens), 1)
    same = t_out // group_len == t_in // group_len
    within = jnp.where(also(same, t_out >= t_in), 1.0, 0.0).astype(jnp.bfloat16)

    def compute(d, r, lo, size):
        x = raw[r // head_rows, d, lax.rem(r, head_rows), pl.ds(lo, size), :]
        x = x.astype(jnp.float32).astype(jnp.bfloat16)
        run = jnp.dot(within[:size, :size], x, preferred_element_type=jnp.float32)
        sums[d, r, pl.ds(lo, size), :] = run.astype(jnp.bfloat16)

    def moves(own):
        up = zone // half < own // half
        last = also(zone == grps - 1, lax.rem(own, half) == half - 1)
        return jnp.logical_or(up, lax.rem(own, half) == 0)

    def is_moved(own, e, i, lo, size):
        hit = size == piece and e == 0 and lo // piece in MOVED
        return also(i == 0, moves(own)) if hit else i < 0

    def send_all(i, r, lo, size):
        def compute_all():
            for side in range(2):
                for e in range(half):
                    compute((i * half + e) * 2 + side, r, lo, size)

        if size == piece and lo == 0:
            pl.when(i > 0)(compute_all)
        else:
            compute_all()

        for e in range(half):
            d = (i * half + e) * 2
            relayed = also(via, jnp.logical_not(is_moved(g, e, i, lo, size)))

            @pl.when(relayed)
            def _(d=d):
                send_relay(d, r, lo, size).start()

            @pl.when(jnp.logical_not(relayed))
            def _(d=d):
                send_part(d, r, lo, size).start()

        for e in range(half):
            d = (i * half + e) * 2 + 1

            @pl.when(jnp.logical_not(is_me(d)))
            def _(d=d):
                send_part(d, r, lo, size).start()

    def forward_all(i, r, lo, size):
        def from_relay(e):
            d = (i * half + e) * 2
            forward(d, r, lo, size).start()

        if size == tokens:
            both = relay.at[pl.ds(i * half, half), r]
            here(both, relay_sem.at[i, r - 1]).wait_recv()
            for e in range(half):
                from_relay(e)
        else:
            for e in range(half):
                @pl.when(jnp.logical_not(is_moved(partner, e, i, lo, size)))
                def _(e=e):
                    send_relay((i * half + e) * 2, r, lo, size).wait_recv()
                    from_relay(e)

    lane = lax.broadcasted_iota(jnp.int32, (groups, rows * groups), 1)
    spread = (lax.rem(lane, groups) == lax.broadcasted_iota(jnp.int32, lane.shape, 0))
    lane = lax.broadcasted_iota(jnp.int32, (rows, rows * groups), 1)
    own_row = lane // groups == lax.broadcasted_iota(jnp.int32, lane.shape, 0)

    def send_small():
        fetch_index.wait()
        fetch_anchor.wait()

        ids = index_ref[...].astype(jnp.float32).astype(jnp.bfloat16)
        ids = ids.reshape(-1, groups)
        wide = jnp.dot(ids, spread.astype(jnp.bfloat16), preferred_element_type=jnp.float32)
        wide_ref[...] = wide.reshape(wide_ref.shape)

        @pl.loop(0, blocks)
        def _(d):
            _, _, b0, k0 = place_from(d, g)
            line = 0.0
            for b in range(seq_rows):
                these = pl.ds(b * head_rows, head_rows)
                anchor_out[d, these, :] = anchor_ref[b0 + b, pl.ds(k0, head_rows), :]
                kept = jnp.where(own_row[b * head_rows:(b + 1) * head_rows],
                                 wide_ref[b0 + b, pl.ds(k0, head_rows), :], 0.0)
                line += jnp.sum(kept, axis=0, keepdims=True)
            index_out[d] = line.astype(jnp.int32)

            relayed = also(lax.rem(d, 2) == 0, via)

            @pl.when(relayed)
            def _():
                hold_index(d).start()

            @pl.when(jnp.logical_not(jnp.logical_or(relayed, is_me(d))))
            def _():
                send_index(d).start()

            @pl.when(sends_anchor(d))
            def _():
                send_anchor(d).start()

    steps = (chunks + LEAD * (per_grp - 1)) * per_grp
    first_loaded(0, 1, first_sem).wait()
    for d in range(ahead):
        compute(d, 0, 0, piece)
    pl.semaphore_wait(barrier, expected)

    def at_chunk(n, ready, do):
        i = lax.rem(n, per_grp)
        c = n // per_grp - LEAD * i
        for lo in (0, piece):
            @pl.when(also(ready, c == lo // piece))
            def _(lo=lo):
                do(i, 0, lo, piece)

        @pl.when(also(ready, also(c >= 2, c < chunks)))
        def _():
            do(i, c - 1, 0, tokens)

    def wait_and_send(i, r, lo, size):
        if lo == 0:
            if head_rows > 1:
                @pl.when(also(i == 0, r == 1))
                def _():
                    first_loaded(1, head_rows - 1, rest_sem).wait()

            for b in range(seq_rows):
                for k in range(1 if b == 0 else 0, per_grp):
                    @pl.when(also(i == k, r == b * head_rows))
                    def _(b=b, k=k):
                        loaded(b, k).wait()
        send_all(i, r, lo, size)

    lag = jnp.where(zone // half == g // half, RELAY_LAG, LAG)

    @pl.loop(0, steps + LAG)
    def _(n):
        m = n - lag
        at_chunk(jnp.maximum(m, 0), also(also(m >= 0, m < steps), pass_on), forward_all)
        at_chunk(n, n < steps, wait_and_send)

        @pl.when(n == SMALL)
        def _():
            send_small()

        @pl.when(also(pass_on, n == SMALL + LAG))
        def _():
            here(index_hold, ihold_sem).wait_recv()

            @pl.loop(0, blocks // 2)
            def _(e):
                forward_index(e * 2).start()

    fetch_table = pltpu.make_async_copy(table_hbm, table_ref, small_sem.at[0])
    fetch_scale = pltpu.make_async_copy(anchor_scale_hbm, anchor_scale_ref, small_sem.at[1])
    fetch_table.start()
    fetch_scale.start()

    @pl.loop(0, blocks)
    def _(d):
        @pl.when(is_me(d))
        def _():
            index_in[s] = index_out[d]
            anchor_in[...] = anchor_out[d]
            for r in range(rows):
                landed[r, pl.ds(pl.multiple_of(s * tokens, tokens), tokens), :] = sums[d, r]

    def fewer(part, size, sem):
        @pl.when(mine)
        def _():
            here(part(size - size // seqs), sem).wait_recv()

        @pl.when(jnp.logical_not(mine))
        def _():
            here(part(size), sem).wait_recv()

    @pl.when(jnp.logical_not(mine))
    def _():
        here(anchor_in, arecv_sem).wait_recv()

    fetch_table.wait()
    fetch_scale.wait()
    for r in range(rows):
        base_ref[r] = anchor_in[pl.ds(r, 1), :].astype(jnp.float32) * anchor_scale_ref[...]

    fewer(lambda size: index_in.at[pl.ds(0, size)], seqs, irecv_sem)

    @pl.loop(0, seqs)
    def _(j):
        many = rows * groups
        ids = jnp.broadcast_to(index_in[j], (levels, many))
        hot = (ids == lax.broadcasted_iota(jnp.int32, (levels, many), 0)).astype(jnp.float32)
        found = lax.dot_general(
            hot, table_ref[...], (((0,), (0,)), ((), ())),
            precision=HIGHEST, preferred_element_type=jnp.float32,
        )
        for r in range(rows):
            scales_ref[r, pl.ds(pl.multiple_of(j * groups, groups), groups), :] = (
                found[r * groups:(r + 1) * groups]
            )

    def finish(group, first, last):
        many_rows = pl.ds(first, last - first)
        fewer(lambda size: landed.at[many_rows, pl.ds(0, size)], seqs * tokens, recv_sem.at[group])

        @pl.loop(first, min(last, rows - min(KEEP, rows)))
        def _(r):
            many, step = grow(landed, scales_ref, base_ref, r)

            def put(j, base):
                at, built, base = step(j, base)
                landed[r, pl.ds(at, group_len), :] = built
                return base

            lax.fori_loop(0, many, put, base_ref[r], unroll=16)

    for group, first in enumerate(cuts[:-1]):
        finish(group, first, cuts[group + 1])

    def sent(ref):
        here(ref, recv_sem.at[0]).wait_send()

    @pl.when(mine)
    def _():
        sent(sums.at[pl.ds(0, blocks - 1)])
        sent(index_out.at[pl.ds(0, blocks - 1)])
        for _ in range(grps - 1):
            sent(anchor_out.at[0])

    @pl.when(jnp.logical_not(mine))
    def _():
        sent(sums)
        sent(index_out)

    @pl.when(pass_on)
    def _():
        sent(index_hold)
        if MOVED:
            sent(relay.at[pl.ds(1, blocks // 2 - 1)])
            if rows > 1:
                sent(relay.at[0, pl.ds(1, rows - 1)])
            for k in range(2):
                @pl.when(jnp.logical_not(is_moved(partner, 0, 0, k * piece, piece)))
                def _(k=k):
                    sent(relay.at[0, 0, pl.ds(k * piece, piece)])
        else:
            sent(relay)


def rebuild(landed, scales_ref, base_ref, out_hbm, built, out_sem):
    rows = landed.shape[0]
    keep = built.shape[0]
    done = rows - keep
    stores = []
    if done:
        these = pl.ds(0, done)
        stores.append(pltpu.make_async_copy(landed.at[these], out_hbm.at[0, these], out_sem.at[keep]))
        stores[0].start()
    for q in range(keep):
        r = done + q
        many, step = grow(landed, scales_ref, base_ref, r)
        group_len = landed.shape[1] // many

        def put(j, base, q=q, step=step):
            at, grown, base = step(j, base)
            built[q, pl.ds(at, group_len), :] = grown
            return base

        lax.fori_loop(0, many, put, base_ref[r], unroll=16)
        stores.append(pltpu.make_async_copy(built.at[q], out_hbm.at[0, r], out_sem.at[q]))
        stores[-1].start()
    for store in stores:
        store.wait()


def on_device(delta_codes, scale_index, anchor_codes, scale_table, anchor_scale):
    seqs, grps = lax.axis_size("seq"), lax.axis_size("grp")
    seq_local, kv_heads, tokens, channels = delta_codes.shape
    groups = scale_index.shape[2]
    heads = kv_heads // grps
    rows = seq_local * grps * heads // seqs
    blocks = seq_local * kv_heads // rows
    seq_rows, head_rows = max(1, rows // heads), min(rows, heads)
    keep = min(KEEP, rows)
    length = seqs * tokens
    vmem = pl.BlockSpec(memory_space=pltpu.VMEM)
    hbm = pl.BlockSpec(memory_space=pltpu.HBM)
    operands = (delta_codes, scale_index, anchor_codes, scale_table, anchor_scale[None])
    landed, scales, base = pl.pallas_call(
        exchange,
        out_shape=(
            jax.ShapeDtypeStruct((rows, length, channels), jnp.bfloat16),
            jax.ShapeDtypeStruct((rows, seqs * groups, channels), jnp.float32),
            jax.ShapeDtypeStruct((rows, 1, channels), jnp.float32),
        ),
        in_specs=[hbm] * 5,
        out_specs=(vmem, vmem, vmem),
        scratch_shapes=[
            pltpu.VMEM((seq_rows, blocks, head_rows, tokens, channels), jnp.int32),
            pltpu.VMEM((blocks, rows, tokens, channels), jnp.bfloat16),
            pltpu.VMEM((blocks // 2, rows, tokens, channels), jnp.bfloat16),
            pltpu.VMEM((blocks, 1, rows * groups), jnp.int32),
            pltpu.VMEM((blocks // 2, 1, rows * groups), jnp.int32),
            pltpu.VMEM((seqs, 1, rows * groups), jnp.int32),
            pltpu.VMEM((blocks, rows, channels), jnp.int32),
            pltpu.VMEM((rows, channels), jnp.int32),
            pltpu.SemaphoreType.DMA,
            pltpu.SemaphoreType.DMA,
            pltpu.SemaphoreType.DMA((seq_rows, blocks // grps)),
            pltpu.SemaphoreType.DMA,
            pltpu.SemaphoreType.DMA((len(arrival_cuts(rows)) - 1,)),
            pltpu.SemaphoreType.DMA,
            pltpu.SemaphoreType.DMA,
            pltpu.SemaphoreType.DMA,
            pltpu.SemaphoreType.DMA((blocks // 2, 2)),
            pltpu.SemaphoreType.DMA((blocks // grps, max(1, rows - 1))),
            pltpu.VMEM(scale_index.shape, jnp.int32),
            pltpu.VMEM(anchor_codes.shape, jnp.int32),
            pltpu.VMEM(scale_table.shape, jnp.float32),
            pltpu.VMEM((1, channels), jnp.float32),
            pltpu.SemaphoreType.DMA((2,)),
            pltpu.VMEM(scale_index.shape[:2] + (rows * groups,), jnp.float32),
        ],
        compiler_params=pltpu.CompilerParams(
            collective_id=0, has_side_effects=True, vmem_limit_bytes=48 * 1024 * 1024
        ),
        name="exchange",
    )(*(pltpu.with_memory_space_constraint(x, pltpu.HBM) for x in operands))

    return pl.pallas_call(
        rebuild,
        out_shape=jax.ShapeDtypeStruct((1, rows, length, channels), jnp.bfloat16),
        in_specs=[vmem] * 3,
        out_specs=hbm,
        scratch_shapes=[
            pltpu.VMEM((keep, length, channels), jnp.bfloat16),
            pltpu.SemaphoreType.DMA((keep + 1,)),
        ],
        compiler_params=pltpu.CompilerParams(vmem_limit_bytes=16 * 1024 * 1024),
        name="rebuild",
    )(landed, scales, base)


def solution(mesh):
    placed = (P("grp", None, "seq", None), P("grp", None, "seq"), P("grp", None, None), P(), P())
    return jax.shard_map(
        on_device,
        mesh=mesh,
        in_specs=placed,
        out_specs=P("grp", "seq", None, None),
        check_vma=False,
    )
```

```python
import jax
import jax.numpy as jnp
from jax import lax
from jax.experimental import pallas as pl
from jax.experimental.pallas import tpu as pltpu
from jax.sharding import PartitionSpec as P

MESH = pl.DeviceIdType.MESH
MOVED = (1,)
SMALL = 6
LEAD = 0
LAG = 4
FIRST = 2
RELAY_LAG = 1
KEEP = 1
HIGHEST = lax.Precision.HIGHEST


def grow(landed, scales_ref, base_ref, r):
    groups = scales_ref.shape[1]
    group_len = landed.shape[1] // groups

    def step(j, base):
        at = pl.multiple_of(j * group_len, group_len)
        x = landed[r, pl.ds(at, group_len), :].astype(jnp.float32)
        grown = x * scales_ref[r, pl.ds(j, 1), :]
        return at, (grown + base).astype(jnp.bfloat16), base + grown[group_len - 1:]

    return groups, step


def arrival_cuts(rows):
    return sorted({0, rows // 2, rows - min(KEEP, rows), rows})


def exchange(
    codes, index_hbm, anchor_hbm, table_hbm, anchor_scale_hbm,
    landed, scales_ref, base_ref,
    raw, sums, relay, index_out, index_hold, index_in, anchor_out, anchor_in,
    first_sem, rest_sem, load_sem, send_sem, recv_sem, ihold_sem, irecv_sem, arecv_sem,
    relay_half_sem, relay_sem,
    index_ref, anchor_ref, table_ref, anchor_scale_ref, small_sem, wide_ref,
):
    seqs, grps = lax.axis_size("seq"), lax.axis_size("grp")
    s, g = lax.axis_index("seq"), lax.axis_index("grp")
    blocks, rows, tokens, channels = sums.shape
    heads = codes.shape[1] // grps
    per_grp = blocks // grps
    half = grps // 2
    partner = lax.rem(g + half, grps)
    seq_rows, head_rows = raw.shape[0], raw.shape[2]
    levels = table_ref.shape[0]
    groups = index_hbm.shape[2]
    group_len = tokens // groups
    piece = tokens // FIRST
    halves = ((0, piece), (piece, tokens - piece))
    zone = s // per_grp
    zone_partner = lax.rem(zone + half, grps)
    via = zone != g
    pass_on = zone != partner
    mine = zone == g
    also = jnp.logical_and
    chunks = rows + 1
    cuts = arrival_cuts(rows)

    def arrival_sem(r):
        group = 0
        for at in cuts[1:-1]:
            group = group + jnp.where(r >= at, 1, 0)
        return recv_sem.at[group]


    def place_from(d, own):
        side, e, i = lax.rem(d, 2), lax.rem(d // 2, half), d // 2 // half
        h = lax.rem(own // half + 1 + side, 2) * half + lax.rem(e + i, half)
        first = i * rows
        return h, own * per_grp + i, first // heads, h * heads + lax.rem(first, heads)

    def is_me(d):
        h, to_s, _, _ = place_from(d, g)
        return also(h == g, to_s == s)

    def load(d, b, sem):
        _, _, b0, k0 = place_from(d, g)
        return pltpu.make_async_copy(codes.at[b0 + b, pl.ds(k0, head_rows)], raw.at[b, d], sem)

    def loaded(b, i):
        these = raw.at[b, pl.ds(i * 2 * half, 2 * half)]
        return pltpu.make_async_copy(these, these, load_sem.at[b, i])

    def spot(r, lo, size):
        return landed.at[r, pl.ds(pl.multiple_of(s * tokens + lo, piece), size), :]

    def remote(src, dst, rsem, h, to_s):
        return pltpu.make_async_remote_copy(
            src_ref=src, dst_ref=dst, send_sem=send_sem, recv_sem=rsem,
            device_id={"seq": to_s, "grp": h}, device_id_type=MESH,
        )

    def here(ref, rsem):
        return remote(ref, ref, rsem, g, s)

    def relay_sem_at(d, r, lo, size):
        if size == tokens:
            return relay_sem.at[d // 2 // half, r - 1]
        return relay_half_sem.at[d // 2, 1 if lo else 0]

    def send_relay(d, r, lo, size):
        return remote(
            sums.at[d, r, pl.ds(lo, size)], relay.at[d // 2, r, pl.ds(lo, size)],
            relay_sem_at(d, r, lo, size), partner, s,
        )

    def send_part(d, r, lo, size):
        h, to_s, _, _ = place_from(d, g)
        return remote(sums.at[d, r, pl.ds(lo, size)], spot(r, lo, size), arrival_sem(r), h, to_s)

    def forward(d, r, lo, size):
        h, to_s, _, _ = place_from(d, partner)
        return remote(
            relay.at[d // 2, r, pl.ds(lo, size)], spot(r, lo, size), arrival_sem(r), h, to_s
        )

    def send_index(d):
        h, to_s, _, _ = place_from(d, g)
        return remote(index_out.at[d], index_in.at[s], irecv_sem, h, to_s)

    def hold_index(d):
        return remote(index_out.at[d], index_hold.at[d // 2], ihold_sem, partner, s)

    def forward_index(d):
        h, to_s, _, _ = place_from(d, partner)
        return remote(index_hold.at[d // 2], index_in.at[s], irecv_sem, h, to_s)

    def send_anchor(d):
        h, to_s, _, _ = place_from(d, g)
        return remote(anchor_out.at[d], anchor_in, arecv_sem, h, to_s)

    def sends_anchor(d):
        _, to_s, _, _ = place_from(d, g)
        return also(to_s == s, jnp.logical_not(is_me(d)))

    ahead = 2 * half

    def first_rows(d, lo, size, sem):
        _, _, b0, k0 = place_from(d, g)
        return pltpu.make_async_copy(
            codes.at[b0, pl.ds(k0 + lo, size)], raw.at[0, d, pl.ds(lo, size)], sem
        )

    def first_loaded(lo, size, sem):
        these = raw.at[0, pl.ds(0, ahead), pl.ds(lo, size)]
        return pltpu.make_async_copy(these, these, sem)

    barrier = pltpu.get_barrier_semaphore()

    @pl.when(pass_on)
    def _():
        pl.semaphore_signal(
            barrier, inc=1, device_id={"seq": s, "grp": partner}, device_id_type=MESH
        )


    @pl.loop(0, seqs)
    def _(j):
        straight = jnp.logical_or(zone // half == g // half, j // per_grp == zone)
        to_g = jnp.where(straight, zone, zone_partner)

        @pl.when(jnp.logical_not(also(j == s, to_g == g)))
        def _():
            pl.semaphore_signal(
                barrier, inc=1, device_id={"seq": j, "grp": to_g}, device_id_type=MESH
            )

    gets_moved = also(g // half == zone_partner // half, lax.rem(g, half) == 0)

    @pl.when(also(gets_moved, lax.rem(s, per_grp) == 0))
    def _():
        @pl.loop(0, seqs if MOVED else 0)
        def _(j):
            @pl.when(j // per_grp != zone)
            def _():
                pl.semaphore_signal(
                    barrier, inc=1, device_id={"seq": j, "grp": zone}, device_id_type=MESH
                )

    for d in range(ahead):
        first_rows(d, 0, 1, first_sem).start()

    expected = (
        blocks // 2
        + jnp.where(via, 1 + (1 if MOVED else 0), blocks // 2 - 1)
        + jnp.where(pass_on, blocks // 2, 0)
    )

    if head_rows > 1:
        for d in range(ahead):
            first_rows(d, 1, head_rows - 1, rest_sem).start()

    for b in range(seq_rows):
        @pl.loop(ahead if b == 0 else 0, blocks)
        def _(d, b=b):
            load(d, b, load_sem.at[b, d // (2 * half)]).start()

    fetch_index = pltpu.make_async_copy(index_hbm, index_ref, small_sem.at[0])
    fetch_anchor = pltpu.make_async_copy(anchor_hbm, anchor_ref, small_sem.at[1])
    fetch_index.start()
    fetch_anchor.start()

    t_out = lax.broadcasted_iota(jnp.int32, (tokens, tokens), 0)
    t_in = lax.broadcasted_iota(jnp.int32, (tokens, tokens), 1)
    same = t_out // group_len == t_in // group_len
    within = jnp.where(also(same, t_out >= t_in), 1.0, 0.0).astype(jnp.bfloat16)

    def compute(d, r, lo, size):
        x = raw[r // head_rows, d, lax.rem(r, head_rows), pl.ds(lo, size), :]
        x = x.astype(jnp.float32).astype(jnp.bfloat16)
        run = jnp.dot(within[:size, :size], x, preferred_element_type=jnp.float32)
        sums[d, r, pl.ds(lo, size), :] = run.astype(jnp.bfloat16)

    def moves(own):
        up = zone // half < own // half
        last = also(zone == grps - 1, lax.rem(own, half) == half - 1)
        return jnp.logical_or(up, lax.rem(own, half) == 0)

    def is_moved(own, e, i, lo, size):
        hit = size < tokens and e == 0 and (1 if lo else 0) in MOVED
        return also(i == 0, moves(own)) if hit else i < 0

    def send_all(i, r, lo, size):
        def compute_all():
            for side in range(2):
                for e in range(half):
                    compute((i * half + e) * 2 + side, r, lo, size)

        if size < tokens and lo == 0:
            pl.when(i > 0)(compute_all)
        else:
            compute_all()

        for e in range(half):
            d = (i * half + e) * 2
            relayed = also(via, jnp.logical_not(is_moved(g, e, i, lo, size)))

            @pl.when(relayed)
            def _(d=d):
                send_relay(d, r, lo, size).start()

            @pl.when(jnp.logical_not(relayed))
            def _(d=d):
                send_part(d, r, lo, size).start()

        for e in range(half):
            d = (i * half + e) * 2 + 1

            @pl.when(jnp.logical_not(is_me(d)))
            def _(d=d):
                send_part(d, r, lo, size).start()

    def forward_all(i, r, lo, size):
        def from_relay(e):
            d = (i * half + e) * 2
            forward(d, r, lo, size).start()

        if size == tokens:
            both = relay.at[pl.ds(i * half, half), r]
            here(both, relay_sem.at[i, r - 1]).wait_recv()
            for e in range(half):
                from_relay(e)
        else:
            for e in range(half):
                @pl.when(jnp.logical_not(is_moved(partner, e, i, lo, size)))
                def _(e=e):
                    send_relay((i * half + e) * 2, r, lo, size).wait_recv()
                    from_relay(e)

    lane = lax.broadcasted_iota(jnp.int32, (groups, rows * groups), 1)
    spread = (lax.rem(lane, groups) == lax.broadcasted_iota(jnp.int32, lane.shape, 0))
    lane = lax.broadcasted_iota(jnp.int32, (rows, rows * groups), 1)
    own_row = lane // groups == lax.broadcasted_iota(jnp.int32, lane.shape, 0)

    def send_small():
        fetch_index.wait()
        fetch_anchor.wait()

        ids = index_ref[...].astype(jnp.float32).astype(jnp.bfloat16)
        ids = ids.reshape(-1, groups)
        wide = jnp.dot(ids, spread.astype(jnp.bfloat16), preferred_element_type=jnp.float32)
        wide_ref[...] = wide.reshape(wide_ref.shape)

        @pl.loop(0, blocks)
        def _(d):
            _, _, b0, k0 = place_from(d, g)
            line = 0.0
            for b in range(seq_rows):
                these = pl.ds(b * head_rows, head_rows)
                anchor_out[d, these, :] = anchor_ref[b0 + b, pl.ds(k0, head_rows), :]
                kept = jnp.where(own_row[b * head_rows:(b + 1) * head_rows],
                                 wide_ref[b0 + b, pl.ds(k0, head_rows), :], 0.0)
                line += jnp.sum(kept, axis=0, keepdims=True)
            index_out[d] = line.astype(jnp.int32)

            relayed = also(lax.rem(d, 2) == 0, via)

            @pl.when(relayed)
            def _():
                hold_index(d).start()

            @pl.when(jnp.logical_not(jnp.logical_or(relayed, is_me(d))))
            def _():
                send_index(d).start()

            @pl.when(sends_anchor(d))
            def _():
                send_anchor(d).start()

    steps = (chunks + LEAD * (per_grp - 1)) * per_grp
    small_at = min(SMALL, steps - 1)
    first_loaded(0, 1, first_sem).wait()
    for d in range(ahead):
        compute(d, 0, 0, piece)
    pl.semaphore_wait(barrier, expected)

    def at_chunk(n, ready, do):
        i = lax.rem(n, per_grp)
        c = n // per_grp - LEAD * i
        for k, (lo, size) in enumerate(halves):
            @pl.when(also(ready, c == k))
            def _(lo=lo, size=size):
                do(i, 0, lo, size)

        @pl.when(also(ready, also(c >= 2, c < chunks)))
        def _():
            do(i, c - 1, 0, tokens)

    def wait_and_send(i, r, lo, size):
        if lo == 0:
            if head_rows > 1:
                @pl.when(also(i == 0, r == 1))
                def _():
                    first_loaded(1, head_rows - 1, rest_sem).wait()

            for b in range(seq_rows):
                for k in range(1 if b == 0 else 0, per_grp):
                    @pl.when(also(i == k, r == b * head_rows))
                    def _(b=b, k=k):
                        loaded(b, k).wait()
        send_all(i, r, lo, size)

    lag = jnp.where(zone // half == g // half, RELAY_LAG, LAG)

    @pl.loop(0, steps + LAG)
    def _(n):
        m = n - lag
        at_chunk(jnp.maximum(m, 0), also(also(m >= 0, m < steps), pass_on), forward_all)
        at_chunk(n, n < steps, wait_and_send)

        @pl.when(n == small_at)
        def _():
            send_small()

        @pl.when(also(pass_on, n == small_at + LAG))
        def _():
            here(index_hold, ihold_sem).wait_recv()

            @pl.loop(0, blocks // 2)
            def _(e):
                forward_index(e * 2).start()

    fetch_table = pltpu.make_async_copy(table_hbm, table_ref, small_sem.at[0])
    fetch_scale = pltpu.make_async_copy(anchor_scale_hbm, anchor_scale_ref, small_sem.at[1])
    fetch_table.start()
    fetch_scale.start()

    @pl.loop(0, blocks)
    def _(d):
        @pl.when(is_me(d))
        def _():
            index_in[s] = index_out[d]
            anchor_in[...] = anchor_out[d]
            for r in range(rows):
                landed[r, pl.ds(pl.multiple_of(s * tokens, tokens), tokens), :] = sums[d, r]

    def fewer(part, size, sem):
        @pl.when(mine)
        def _():
            here(part(size - size // seqs), sem).wait_recv()

        @pl.when(jnp.logical_not(mine))
        def _():
            here(part(size), sem).wait_recv()

    @pl.when(jnp.logical_not(mine))
    def _():
        here(anchor_in, arecv_sem).wait_recv()

    fetch_table.wait()
    fetch_scale.wait()
    for r in range(rows):
        base_ref[r] = anchor_in[pl.ds(r, 1), :].astype(jnp.float32) * anchor_scale_ref[...]

    fewer(lambda size: index_in.at[pl.ds(0, size)], seqs, irecv_sem)

    @pl.loop(0, seqs)
    def _(j):
        many = rows * groups
        ids = jnp.broadcast_to(index_in[j], (levels, many))
        hot = (ids == lax.broadcasted_iota(jnp.int32, (levels, many), 0)).astype(jnp.float32)
        found = lax.dot_general(
            hot, table_ref[...], (((0,), (0,)), ((), ())),
            precision=HIGHEST, preferred_element_type=jnp.float32,
        )
        for r in range(rows):
            scales_ref[r, pl.ds(pl.multiple_of(j * groups, groups), groups), :] = (
                found[r * groups:(r + 1) * groups]
            )

    def finish(group, first, last):
        many_rows = pl.ds(first, last - first)
        fewer(lambda size: landed.at[many_rows, pl.ds(0, size)], seqs * tokens, recv_sem.at[group])

        @pl.loop(first, min(last, rows - min(KEEP, rows)))
        def _(r):
            many, step = grow(landed, scales_ref, base_ref, r)

            def put(j, base):
                at, built, base = step(j, base)
                landed[r, pl.ds(at, group_len), :] = built
                return base

            lax.fori_loop(0, many, put, base_ref[r], unroll=16)

    for group, first in enumerate(cuts[:-1]):
        finish(group, first, cuts[group + 1])

    def sent(ref):
        here(ref, recv_sem.at[0]).wait_send()

    @pl.when(mine)
    def _():
        sent(sums.at[pl.ds(0, blocks - 1)])
        sent(index_out.at[pl.ds(0, blocks - 1)])
        for _ in range(grps - 1):
            sent(anchor_out.at[0])

    @pl.when(jnp.logical_not(mine))
    def _():
        sent(sums)
        sent(index_out)

    @pl.when(pass_on)
    def _():
        sent(index_hold)
        if MOVED:
            sent(relay.at[pl.ds(1, blocks // 2 - 1)])
            if rows > 1:
                sent(relay.at[0, pl.ds(1, rows - 1)])
            for lo, size in halves:
                @pl.when(jnp.logical_not(is_moved(partner, 0, 0, lo, size)))
                def _(lo=lo, size=size):
                    sent(relay.at[0, 0, pl.ds(lo, size)])
        else:
            sent(relay)


def rebuild(landed, scales_ref, base_ref, out_hbm, built, out_sem):
    rows = landed.shape[0]
    keep = built.shape[0]
    done = rows - keep
    stores = []
    if done:
        these = pl.ds(0, done)
        stores.append(pltpu.make_async_copy(landed.at[these], out_hbm.at[0, these], out_sem.at[keep]))
        stores[0].start()
    for q in range(keep):
        r = done + q
        many, step = grow(landed, scales_ref, base_ref, r)
        group_len = landed.shape[1] // many

        def put(j, base, q=q, step=step):
            at, grown, base = step(j, base)
            built[q, pl.ds(at, group_len), :] = grown
            return base

        lax.fori_loop(0, many, put, base_ref[r], unroll=16)
        stores.append(pltpu.make_async_copy(built.at[q], out_hbm.at[0, r], out_sem.at[q]))
        stores[-1].start()
    for store in stores:
        store.wait()


def on_device(delta_codes, scale_index, anchor_codes, scale_table, anchor_scale):
    seqs, grps = lax.axis_size("seq"), lax.axis_size("grp")
    seq_local, kv_heads, tokens, channels = delta_codes.shape
    groups = scale_index.shape[2]
    heads = kv_heads // grps
    rows = seq_local * grps * heads // seqs
    blocks = seq_local * kv_heads // rows
    seq_rows, head_rows = max(1, rows // heads), min(rows, heads)
    keep = min(KEEP, rows)
    length = seqs * tokens
    vmem = pl.BlockSpec(memory_space=pltpu.VMEM)
    hbm = pl.BlockSpec(memory_space=pltpu.HBM)
    operands = (delta_codes, scale_index, anchor_codes, scale_table, anchor_scale[None])
    landed, scales, base = pl.pallas_call(
        exchange,
        out_shape=(
            jax.ShapeDtypeStruct((rows, length, channels), jnp.bfloat16),
            jax.ShapeDtypeStruct((rows, seqs * groups, channels), jnp.float32),
            jax.ShapeDtypeStruct((rows, 1, channels), jnp.float32),
        ),
        in_specs=[hbm] * 5,
        out_specs=(vmem, vmem, vmem),
        scratch_shapes=[
            pltpu.VMEM((seq_rows, blocks, head_rows, tokens, channels), jnp.int32),
            pltpu.VMEM((blocks, rows, tokens, channels), jnp.bfloat16),
            pltpu.VMEM((blocks // 2, rows, tokens, channels), jnp.bfloat16),
            pltpu.VMEM((blocks, 1, rows * groups), jnp.int32),
            pltpu.VMEM((blocks // 2, 1, rows * groups), jnp.int32),
            pltpu.VMEM((seqs, 1, rows * groups), jnp.int32),
            pltpu.VMEM((blocks, rows, channels), jnp.int32),
            pltpu.VMEM((rows, channels), jnp.int32),
            pltpu.SemaphoreType.DMA,
            pltpu.SemaphoreType.DMA,
            pltpu.SemaphoreType.DMA((seq_rows, blocks // grps)),
            pltpu.SemaphoreType.DMA,
            pltpu.SemaphoreType.DMA((len(arrival_cuts(rows)) - 1,)),
            pltpu.SemaphoreType.DMA,
            pltpu.SemaphoreType.DMA,
            pltpu.SemaphoreType.DMA,
            pltpu.SemaphoreType.DMA((blocks // 2, 2)),
            pltpu.SemaphoreType.DMA((blocks // grps, max(1, rows - 1))),
            pltpu.VMEM(scale_index.shape, jnp.int32),
            pltpu.VMEM(anchor_codes.shape, jnp.int32),
            pltpu.VMEM(scale_table.shape, jnp.float32),
            pltpu.VMEM((1, channels), jnp.float32),
            pltpu.SemaphoreType.DMA((2,)),
            pltpu.VMEM(scale_index.shape[:2] + (rows * groups,), jnp.float32),
        ],
        compiler_params=pltpu.CompilerParams(
            collective_id=0, has_side_effects=True, vmem_limit_bytes=48 * 1024 * 1024
        ),
        name="exchange",
    )(*(pltpu.with_memory_space_constraint(x, pltpu.HBM) for x in operands))

    return pl.pallas_call(
        rebuild,
        out_shape=jax.ShapeDtypeStruct((1, rows, length, channels), jnp.bfloat16),
        in_specs=[vmem] * 3,
        out_specs=hbm,
        scratch_shapes=[
            pltpu.VMEM((keep, length, channels), jnp.bfloat16),
            pltpu.SemaphoreType.DMA((keep + 1,)),
        ],
        compiler_params=pltpu.CompilerParams(vmem_limit_bytes=16 * 1024 * 1024),
        name="rebuild",
    )(landed, scales, base)


def solution(mesh):
    placed = (P("grp", None, "seq", None), P("grp", None, "seq"), P("grp", None, None), P(), P())
    return jax.shard_map(
        on_device,
        mesh=mesh,
        in_specs=placed,
        out_specs=P("grp", "seq", None, None),
        check_vma=False,
    )
```

```python
import jax
import jax.numpy as jnp
from jax import lax
from jax.experimental import pallas as pl
from jax.experimental.pallas import tpu as pltpu
from jax.sharding import PartitionSpec as P

MESH = pl.DeviceIdType.MESH
MOVED = (1,)
SMALL = 6
LEAD = 0
LAG = 4
FIRST = 2
RELAY_LAG = 1
KEEP = 1
HIGHEST = lax.Precision.HIGHEST


def grow(landed, scales_ref, base_ref, r):
    groups = scales_ref.shape[1]
    group_len = landed.shape[1] // groups

    def step(j, base):
        at = pl.multiple_of(j * group_len, group_len)
        x = landed[r, pl.ds(at, group_len), :].astype(jnp.float32)
        grown = x * scales_ref[r, pl.ds(j, 1), :]
        return at, (grown + base).astype(jnp.bfloat16), base + grown[group_len - 1:]

    return groups, step


def arrival_cuts(rows):
    return sorted({0, rows // 2, rows - min(KEEP, rows), rows})


def exchange(
    codes, index_hbm, anchor_hbm, table_hbm, anchor_scale_hbm,
    landed, scales_ref, base_ref,
    raw, sums, relay, index_out, index_hold, index_in, anchor_out, anchor_in,
    first_sem, rest_sem, load_sem, send_sem, recv_sem, ihold_sem, irecv_sem, arecv_sem,
    relay_half_sem, relay_sem,
    index_ref, anchor_ref, table_ref, anchor_scale_ref, small_sem, wide_ref,
):
    seqs, grps = lax.axis_size("seq"), lax.axis_size("grp")
    s, g = lax.axis_index("seq"), lax.axis_index("grp")
    blocks, rows, tokens, channels = sums.shape
    heads = codes.shape[1] // grps
    per_grp = blocks // grps
    half = grps // 2
    partner = lax.rem(g + half, grps)
    seq_rows, head_rows = raw.shape[0], raw.shape[2]
    levels = table_ref.shape[0]
    groups = index_hbm.shape[2]
    group_len = tokens // groups
    piece = tokens // FIRST
    halves = ((0, piece), (piece, tokens - piece))
    zone = s // per_grp
    zone_partner = lax.rem(zone + half, grps)
    via = zone != g
    pass_on = zone != partner
    mine = zone == g
    also = jnp.logical_and
    chunks = rows + 1
    cuts = arrival_cuts(rows)

    def arrival_sem(r):
        group = 0
        for at in cuts[1:-1]:
            group = group + jnp.where(r >= at, 1, 0)
        return recv_sem.at[group]


    def place_from(d, own):
        side, e, i = lax.rem(d, 2), lax.rem(d // 2, half), d // 2 // half
        h = lax.rem(own // half + 1 + side, 2) * half + lax.rem(e + i, half)
        first = i * rows
        return h, own * per_grp + i, first // heads, h * heads + lax.rem(first, heads)

    def is_me(d):
        h, to_s, _, _ = place_from(d, g)
        return also(h == g, to_s == s)

    def load(d, b, sem):
        _, _, b0, k0 = place_from(d, g)
        return pltpu.make_async_copy(codes.at[b0 + b, pl.ds(k0, head_rows)], raw.at[b, d], sem)

    def loaded(b, i):
        these = raw.at[b, pl.ds(i * 2 * half, 2 * half)]
        return pltpu.make_async_copy(these, these, load_sem.at[b, i])

    def spot(r, lo, size):
        return landed.at[r, pl.ds(pl.multiple_of(s * tokens + lo, piece), size), :]

    def remote(src, dst, rsem, h, to_s):
        return pltpu.make_async_remote_copy(
            src_ref=src, dst_ref=dst, send_sem=send_sem, recv_sem=rsem,
            device_id={"seq": to_s, "grp": h}, device_id_type=MESH,
        )

    def here(ref, rsem):
        return remote(ref, ref, rsem, g, s)

    def relay_sem_at(d, r, lo, size):
        if size == tokens:
            return relay_sem.at[d // 2 // half, r - 1]
        return relay_half_sem.at[d // 2, 1 if lo else 0]

    def send_relay(d, r, lo, size):
        return remote(
            sums.at[d, r, pl.ds(lo, size)], relay.at[d // 2, r, pl.ds(lo, size)],
            relay_sem_at(d, r, lo, size), partner, s,
        )

    def send_part(d, r, lo, size):
        h, to_s, _, _ = place_from(d, g)
        return remote(sums.at[d, r, pl.ds(lo, size)], spot(r, lo, size), arrival_sem(r), h, to_s)

    def forward(d, r, lo, size):
        h, to_s, _, _ = place_from(d, partner)
        return remote(
            relay.at[d // 2, r, pl.ds(lo, size)], spot(r, lo, size), arrival_sem(r), h, to_s
        )

    def send_index(d):
        h, to_s, _, _ = place_from(d, g)
        return remote(index_out.at[d], index_in.at[s], irecv_sem, h, to_s)

    def hold_index(d):
        return remote(index_out.at[d], index_hold.at[d // 2], ihold_sem, partner, s)

    def forward_index(d):
        h, to_s, _, _ = place_from(d, partner)
        return remote(index_hold.at[d // 2], index_in.at[s], irecv_sem, h, to_s)

    def send_anchor(d):
        h, to_s, _, _ = place_from(d, g)
        return remote(anchor_out.at[d], anchor_in, arecv_sem, h, to_s)

    def sends_anchor(d):
        _, to_s, _, _ = place_from(d, g)
        return also(to_s == s, jnp.logical_not(is_me(d)))

    ahead = 2 * half

    def first_rows(d, lo, size, sem):
        _, _, b0, k0 = place_from(d, g)
        return pltpu.make_async_copy(
            codes.at[b0, pl.ds(k0 + lo, size)], raw.at[0, d, pl.ds(lo, size)], sem
        )

    def first_loaded(lo, size, sem):
        these = raw.at[0, pl.ds(0, ahead), pl.ds(lo, size)]
        return pltpu.make_async_copy(these, these, sem)

    barrier = pltpu.get_barrier_semaphore()

    @pl.when(pass_on)
    def _():
        pl.semaphore_signal(
            barrier, inc=1, device_id={"seq": s, "grp": partner}, device_id_type=MESH
        )


    @pl.loop(0, seqs)
    def _(j):
        straight = jnp.logical_or(zone // half == g // half, j // per_grp == zone)
        to_g = jnp.where(straight, zone, zone_partner)

        @pl.when(jnp.logical_not(also(j == s, to_g == g)))
        def _():
            pl.semaphore_signal(
                barrier, inc=1, device_id={"seq": j, "grp": to_g}, device_id_type=MESH
            )

    gets_moved = also(g // half == zone_partner // half, lax.rem(g, half) == 0)

    @pl.when(also(gets_moved, lax.rem(s, per_grp) == 0))
    def _():
        @pl.loop(0, seqs if MOVED else 0)
        def _(j):
            @pl.when(j // per_grp != zone)
            def _():
                pl.semaphore_signal(
                    barrier, inc=1, device_id={"seq": j, "grp": zone}, device_id_type=MESH
                )

    for d in range(ahead):
        first_rows(d, 0, 1, first_sem).start()

    expected = (
        blocks // 2
        + jnp.where(via, 1 + (1 if MOVED else 0), blocks // 2 - 1)
        + jnp.where(pass_on, blocks // 2, 0)
    )

    if head_rows > 1:
        for d in range(ahead):
            first_rows(d, 1, head_rows - 1, rest_sem).start()

    for b in range(seq_rows):
        @pl.loop(ahead if b == 0 else 0, blocks)
        def _(d, b=b):
            load(d, b, load_sem.at[b, d // (2 * half)]).start()

    fetch_index = pltpu.make_async_copy(index_hbm, index_ref, small_sem.at[0])
    fetch_anchor = pltpu.make_async_copy(anchor_hbm, anchor_ref, small_sem.at[1])
    fetch_index.start()
    fetch_anchor.start()

    t_out = lax.broadcasted_iota(jnp.int32, (tokens, tokens), 0)
    t_in = lax.broadcasted_iota(jnp.int32, (tokens, tokens), 1)
    same = t_out // group_len == t_in // group_len
    within = jnp.where(also(same, t_out >= t_in), 1.0, 0.0).astype(jnp.bfloat16)

    def compute(d, r, lo, size):
        x = raw[r // head_rows, d, lax.rem(r, head_rows), pl.ds(lo, size), :]
        x = x.astype(jnp.float32).astype(jnp.bfloat16)
        run = jnp.dot(within[:size, :size], x, preferred_element_type=jnp.float32)
        sums[d, r, pl.ds(lo, size), :] = run.astype(jnp.bfloat16)

    def moves(own):
        up = zone // half < own // half
        last = also(zone == grps - 1, lax.rem(own, half) == half - 1)
        return jnp.logical_or(up, lax.rem(own, half) == 0)

    def is_moved(own, e, i, lo, size):
        hit = size < tokens and e == 0 and (1 if lo else 0) in MOVED
        return also(i == 0, moves(own)) if hit else i < 0

    def send_all(i, r, lo, size):
        def compute_all():
            for side in range(2):
                for e in range(half):
                    compute((i * half + e) * 2 + side, r, lo, size)

        if size < tokens and lo == 0:
            pl.when(i > 0)(compute_all)
        else:
            compute_all()

        for e in range(half):
            d = (i * half + e) * 2
            relayed = also(via, jnp.logical_not(is_moved(g, e, i, lo, size)))

            @pl.when(relayed)
            def _(d=d):
                send_relay(d, r, lo, size).start()

            @pl.when(jnp.logical_not(relayed))
            def _(d=d):
                send_part(d, r, lo, size).start()

        for e in range(half):
            d = (i * half + e) * 2 + 1

            @pl.when(jnp.logical_not(is_me(d)))
            def _(d=d):
                send_part(d, r, lo, size).start()

    def forward_all(i, r, lo, size):
        def from_relay(e):
            d = (i * half + e) * 2
            forward(d, r, lo, size).start()

        if size == tokens:
            both = relay.at[pl.ds(i * half, half), r]
            here(both, relay_sem.at[i, r - 1]).wait_recv()
            for e in range(half):
                from_relay(e)
        else:
            for e in range(half):
                @pl.when(jnp.logical_not(is_moved(partner, e, i, lo, size)))
                def _(e=e):
                    send_relay((i * half + e) * 2, r, lo, size).wait_recv()
                    from_relay(e)

    lane = lax.broadcasted_iota(jnp.int32, (groups, rows * groups), 1)
    spread = (lax.rem(lane, groups) == lax.broadcasted_iota(jnp.int32, lane.shape, 0))
    lane = lax.broadcasted_iota(jnp.int32, (rows, rows * groups), 1)
    own_row = lane // groups == lax.broadcasted_iota(jnp.int32, lane.shape, 0)

    def send_small():
        fetch_index.wait()
        fetch_anchor.wait()

        ids = index_ref[...].astype(jnp.float32).astype(jnp.bfloat16)
        ids = ids.reshape(-1, groups)
        wide = jnp.dot(ids, spread.astype(jnp.bfloat16), preferred_element_type=jnp.float32)
        wide_ref[...] = wide.reshape(wide_ref.shape)

        @pl.loop(0, blocks)
        def _(d):
            _, _, b0, k0 = place_from(d, g)
            line = 0.0
            for b in range(seq_rows):
                these = pl.ds(b * head_rows, head_rows)
                anchor_out[d, these, :] = anchor_ref[b0 + b, pl.ds(k0, head_rows), :]
                kept = jnp.where(own_row[b * head_rows:(b + 1) * head_rows],
                                 wide_ref[b0 + b, pl.ds(k0, head_rows), :], 0.0)
                line += jnp.sum(kept, axis=0, keepdims=True)
            index_out[d] = line.astype(jnp.int32)

        @pl.loop(0, blocks)
        def _(d):
            relayed = also(lax.rem(d, 2) == 0, via)

            @pl.when(relayed)
            def _():
                hold_index(d).start()

            @pl.when(jnp.logical_not(jnp.logical_or(relayed, is_me(d))))
            def _():
                send_index(d).start()

            @pl.when(sends_anchor(d))
            def _():
                send_anchor(d).start()

    steps = (chunks + LEAD * (per_grp - 1)) * per_grp
    small_at = min(SMALL, steps - 1)
    first_loaded(0, 1, first_sem).wait()
    for d in range(ahead):
        compute(d, 0, 0, piece)
    pl.semaphore_wait(barrier, expected)

    def at_chunk(n, ready, do):
        i = lax.rem(n, per_grp)
        c = n // per_grp - LEAD * i
        for k, (lo, size) in enumerate(halves):
            @pl.when(also(ready, c == k))
            def _(lo=lo, size=size):
                do(i, 0, lo, size)

        @pl.when(also(ready, also(c >= 2, c < chunks)))
        def _():
            do(i, c - 1, 0, tokens)

    def wait_and_send(i, r, lo, size):
        if lo == 0:
            if head_rows > 1:
                @pl.when(also(i == 0, r == 1))
                def _():
                    first_loaded(1, head_rows - 1, rest_sem).wait()

            for b in range(seq_rows):
                for k in range(1 if b == 0 else 0, per_grp):
                    @pl.when(also(i == k, r == b * head_rows))
                    def _(b=b, k=k):
                        loaded(b, k).wait()
        send_all(i, r, lo, size)

    lag = jnp.where(zone // half == g // half, RELAY_LAG, LAG)

    @pl.loop(0, steps + LAG)
    def _(n):
        m = n - lag
        at_chunk(jnp.maximum(m, 0), also(also(m >= 0, m < steps), pass_on), forward_all)
        at_chunk(n, n < steps, wait_and_send)

        @pl.when(n == small_at)
        def _():
            send_small()

        @pl.when(also(pass_on, n == small_at + LAG))
        def _():
            here(index_hold, ihold_sem).wait_recv()

            @pl.loop(0, blocks // 2)
            def _(e):
                forward_index(e * 2).start()

    fetch_table = pltpu.make_async_copy(table_hbm, table_ref, small_sem.at[0])
    fetch_scale = pltpu.make_async_copy(anchor_scale_hbm, anchor_scale_ref, small_sem.at[1])
    fetch_table.start()
    fetch_scale.start()

    @pl.loop(0, blocks)
    def _(d):
        @pl.when(is_me(d))
        def _():
            index_in[s] = index_out[d]
            anchor_in[...] = anchor_out[d]
            for r in range(rows):
                landed[r, pl.ds(pl.multiple_of(s * tokens, tokens), tokens), :] = sums[d, r]

    def fewer(part, size, sem):
        @pl.when(mine)
        def _():
            here(part(size - size // seqs), sem).wait_recv()

        @pl.when(jnp.logical_not(mine))
        def _():
            here(part(size), sem).wait_recv()

    @pl.when(jnp.logical_not(mine))
    def _():
        here(anchor_in, arecv_sem).wait_recv()

    fetch_table.wait()
    fetch_scale.wait()
    for r in range(rows):
        base_ref[r] = anchor_in[pl.ds(r, 1), :].astype(jnp.float32) * anchor_scale_ref[...]

    fewer(lambda size: index_in.at[pl.ds(0, size)], seqs, irecv_sem)

    @pl.loop(0, seqs)
    def _(j):
        many = rows * groups
        ids = jnp.broadcast_to(index_in[j], (levels, many))
        hot = (ids == lax.broadcasted_iota(jnp.int32, (levels, many), 0)).astype(jnp.float32)
        found = lax.dot_general(
            hot, table_ref[...], (((0,), (0,)), ((), ())),
            precision=HIGHEST, preferred_element_type=jnp.float32,
        )
        for r in range(rows):
            scales_ref[r, pl.ds(pl.multiple_of(j * groups, groups), groups), :] = (
                found[r * groups:(r + 1) * groups]
            )

    def finish(group, first, last):
        many_rows = pl.ds(first, last - first)
        fewer(lambda size: landed.at[many_rows, pl.ds(0, size)], seqs * tokens, recv_sem.at[group])

        @pl.loop(first, min(last, rows - min(KEEP, rows)))
        def _(r):
            many, step = grow(landed, scales_ref, base_ref, r)

            def put(j, base):
                at, built, base = step(j, base)
                landed[r, pl.ds(at, group_len), :] = built
                return base

            lax.fori_loop(0, many, put, base_ref[r], unroll=16)

    for group, first in enumerate(cuts[:-1]):
        finish(group, first, cuts[group + 1])

    def sent(ref):
        here(ref, recv_sem.at[0]).wait_send()

    @pl.when(mine)
    def _():
        sent(sums.at[pl.ds(0, blocks - 1)])
        sent(index_out.at[pl.ds(0, blocks - 1)])
        for _ in range(grps - 1):
            sent(anchor_out.at[0])

    @pl.when(jnp.logical_not(mine))
    def _():
        sent(sums)
        sent(index_out)

    @pl.when(pass_on)
    def _():
        sent(index_hold)
        if MOVED:
            sent(relay.at[pl.ds(1, blocks // 2 - 1)])
            if rows > 1:
                sent(relay.at[0, pl.ds(1, rows - 1)])
            for lo, size in halves:
                @pl.when(jnp.logical_not(is_moved(partner, 0, 0, lo, size)))
                def _(lo=lo, size=size):
                    sent(relay.at[0, 0, pl.ds(lo, size)])
        else:
            sent(relay)


def rebuild(landed, scales_ref, base_ref, out_hbm, built, out_sem):
    rows = landed.shape[0]
    keep = built.shape[0]
    done = rows - keep
    stores = []
    if done:
        these = pl.ds(0, done)
        stores.append(pltpu.make_async_copy(landed.at[these], out_hbm.at[0, these], out_sem.at[keep]))
        stores[0].start()
    for q in range(keep):
        r = done + q
        many, step = grow(landed, scales_ref, base_ref, r)
        group_len = landed.shape[1] // many

        def put(j, base, q=q, step=step):
            at, grown, base = step(j, base)
            built[q, pl.ds(at, group_len), :] = grown
            return base

        lax.fori_loop(0, many, put, base_ref[r], unroll=16)
        stores.append(pltpu.make_async_copy(built.at[q], out_hbm.at[0, r], out_sem.at[q]))
        stores[-1].start()
    for store in stores:
        store.wait()


def on_device(delta_codes, scale_index, anchor_codes, scale_table, anchor_scale):
    seqs, grps = lax.axis_size("seq"), lax.axis_size("grp")
    seq_local, kv_heads, tokens, channels = delta_codes.shape
    groups = scale_index.shape[2]
    heads = kv_heads // grps
    rows = seq_local * grps * heads // seqs
    blocks = seq_local * kv_heads // rows
    seq_rows, head_rows = max(1, rows // heads), min(rows, heads)
    keep = min(KEEP, rows)
    length = seqs * tokens
    vmem = pl.BlockSpec(memory_space=pltpu.VMEM)
    hbm = pl.BlockSpec(memory_space=pltpu.HBM)
    operands = (delta_codes, scale_index, anchor_codes, scale_table, anchor_scale[None])
    landed, scales, base = pl.pallas_call(
        exchange,
        out_shape=(
            jax.ShapeDtypeStruct((rows, length, channels), jnp.bfloat16),
            jax.ShapeDtypeStruct((rows, seqs * groups, channels), jnp.float32),
            jax.ShapeDtypeStruct((rows, 1, channels), jnp.float32),
        ),
        in_specs=[hbm] * 5,
        out_specs=(vmem, vmem, vmem),
        scratch_shapes=[
            pltpu.VMEM((seq_rows, blocks, head_rows, tokens, channels), jnp.int32),
            pltpu.VMEM((blocks, rows, tokens, channels), jnp.bfloat16),
            pltpu.VMEM((blocks // 2, rows, tokens, channels), jnp.bfloat16),
            pltpu.VMEM((blocks, 1, rows * groups), jnp.int32),
            pltpu.VMEM((blocks // 2, 1, rows * groups), jnp.int32),
            pltpu.VMEM((seqs, 1, rows * groups), jnp.int32),
            pltpu.VMEM((blocks, rows, channels), jnp.int32),
            pltpu.VMEM((rows, channels), jnp.int32),
            pltpu.SemaphoreType.DMA,
            pltpu.SemaphoreType.DMA,
            pltpu.SemaphoreType.DMA((seq_rows, blocks // grps)),
            pltpu.SemaphoreType.DMA,
            pltpu.SemaphoreType.DMA((len(arrival_cuts(rows)) - 1,)),
            pltpu.SemaphoreType.DMA,
            pltpu.SemaphoreType.DMA,
            pltpu.SemaphoreType.DMA,
            pltpu.SemaphoreType.DMA((blocks // 2, 2)),
            pltpu.SemaphoreType.DMA((blocks // grps, max(1, rows - 1))),
            pltpu.VMEM(scale_index.shape, jnp.int32),
            pltpu.VMEM(anchor_codes.shape, jnp.int32),
            pltpu.VMEM(scale_table.shape, jnp.float32),
            pltpu.VMEM((1, channels), jnp.float32),
            pltpu.SemaphoreType.DMA((2,)),
            pltpu.VMEM(scale_index.shape[:2] + (rows * groups,), jnp.float32),
        ],
        compiler_params=pltpu.CompilerParams(
            collective_id=0, has_side_effects=True, vmem_limit_bytes=48 * 1024 * 1024
        ),
        name="exchange",
    )(*(pltpu.with_memory_space_constraint(x, pltpu.HBM) for x in operands))

    return pl.pallas_call(
        rebuild,
        out_shape=jax.ShapeDtypeStruct((1, rows, length, channels), jnp.bfloat16),
        in_specs=[vmem] * 3,
        out_specs=hbm,
        scratch_shapes=[
            pltpu.VMEM((keep, length, channels), jnp.bfloat16),
            pltpu.SemaphoreType.DMA((keep + 1,)),
        ],
        compiler_params=pltpu.CompilerParams(vmem_limit_bytes=16 * 1024 * 1024),
        name="rebuild",
    )(landed, scales, base)


def solution(mesh):
    placed = (P("grp", None, "seq", None), P("grp", None, "seq"), P("grp", None, None), P(), P())
    return jax.shard_map(
        on_device,
        mesh=mesh,
        in_specs=placed,
        out_specs=P("grp", "seq", None, None),
        check_vma=False,
    )
```

```python
import jax
import jax.numpy as jnp
from jax import lax
from jax.experimental import pallas as pl
from jax.experimental.pallas import tpu as pltpu
from jax.sharding import PartitionSpec as P

MESH = pl.DeviceIdType.MESH
MOVED = (1,)
SMALL = 6
LEAD = 0
LAG = 3
FIRST = 2
RELAY_LAG = 1
KEEP = 2
HIGHEST = lax.Precision.HIGHEST


def grow(landed, scales_ref, base_ref, r):
    groups = scales_ref.shape[1]
    group_len = landed.shape[1] // groups

    def step(j, base):
        at = pl.multiple_of(j * group_len, group_len)
        x = landed[r, pl.ds(at, group_len), :].astype(jnp.float32)
        grown = x * scales_ref[r, pl.ds(j, 1), :]
        return at, (grown + base).astype(jnp.bfloat16), base + grown[group_len - 1:]

    return groups, step


def arrival_cuts(rows):
    return sorted({0, rows - min(KEEP, rows), rows})


def exchange(
    codes, index_hbm, anchor_hbm, table_hbm, anchor_scale_hbm,
    landed, scales_ref, base_ref,
    raw, sums, relay, index_out, index_hold, index_in, anchor_out, anchor_in,
    first_sem, rest_sem, load_sem, send_sem, recv_sem, ihold_sem, irecv_sem, arecv_sem,
    relay_half_sem, relay_sem,
    index_ref, anchor_ref, table_ref, anchor_scale_ref, small_sem, wide_ref,
):
    seqs, grps = lax.axis_size("seq"), lax.axis_size("grp")
    s, g = lax.axis_index("seq"), lax.axis_index("grp")
    blocks, rows, tokens, channels = sums.shape
    heads = codes.shape[1] // grps
    per_grp = blocks // grps
    half = grps // 2
    partner = lax.rem(g + half, grps)
    seq_rows, head_rows = raw.shape[0], raw.shape[2]
    levels = table_ref.shape[0]
    groups = index_hbm.shape[2]
    group_len = tokens // groups
    piece = tokens // FIRST
    halves = ((0, piece), (piece, tokens - piece))
    zone = s // per_grp
    zone_partner = lax.rem(zone + half, grps)
    via = zone != g
    pass_on = zone != partner
    mine = zone == g
    also = jnp.logical_and
    chunks = rows + 1
    cuts = arrival_cuts(rows)

    def arrival_sem(r):
        group = 0
        for at in cuts[1:-1]:
            group = group + jnp.where(r >= at, 1, 0)
        return recv_sem.at[group]


    def place_from(d, own):
        side, e, i = lax.rem(d, 2), lax.rem(d // 2, half), d // 2 // half
        h = lax.rem(own // half + 1 + side, 2) * half + lax.rem(e + i, half)
        first = i * rows
        return h, own * per_grp + i, first // heads, h * heads + lax.rem(first, heads)

    def is_me(d):
        h, to_s, _, _ = place_from(d, g)
        return also(h == g, to_s == s)

    def load(d, b, sem):
        _, _, b0, k0 = place_from(d, g)
        return pltpu.make_async_copy(codes.at[b0 + b, pl.ds(k0, head_rows)], raw.at[b, d], sem)

    def loaded(b, i):
        these = raw.at[b, pl.ds(i * 2 * half, 2 * half)]
        return pltpu.make_async_copy(these, these, load_sem.at[b, i])

    def spot(r, lo, size):
        return landed.at[r, pl.ds(pl.multiple_of(s * tokens + lo, piece), size), :]

    def remote(src, dst, rsem, h, to_s):
        return pltpu.make_async_remote_copy(
            src_ref=src, dst_ref=dst, send_sem=send_sem, recv_sem=rsem,
            device_id={"seq": to_s, "grp": h}, device_id_type=MESH,
        )

    def here(ref, rsem):
        return remote(ref, ref, rsem, g, s)

    def relay_sem_at(d, r, lo, size):
        if size == tokens:
            return relay_sem.at[d // 2 // half, r - 1]
        return relay_half_sem.at[d // 2, 1 if lo else 0]

    def send_relay(d, r, lo, size):
        return remote(
            sums.at[d, r, pl.ds(lo, size)], relay.at[d // 2, r, pl.ds(lo, size)],
            relay_sem_at(d, r, lo, size), partner, s,
        )

    def send_part(d, r, lo, size):
        h, to_s, _, _ = place_from(d, g)
        return remote(sums.at[d, r, pl.ds(lo, size)], spot(r, lo, size), arrival_sem(r), h, to_s)

    def forward(d, r, lo, size):
        h, to_s, _, _ = place_from(d, partner)
        return remote(
            relay.at[d // 2, r, pl.ds(lo, size)], spot(r, lo, size), arrival_sem(r), h, to_s
        )

    def send_index(d):
        h, to_s, _, _ = place_from(d, g)
        return remote(index_out.at[d], index_in.at[s], irecv_sem, h, to_s)

    def hold_index(d):
        return remote(index_out.at[d], index_hold.at[d // 2], ihold_sem, partner, s)

    def forward_index(d):
        h, to_s, _, _ = place_from(d, partner)
        return remote(index_hold.at[d // 2], index_in.at[s], irecv_sem, h, to_s)

    def send_anchor(d):
        h, to_s, _, _ = place_from(d, g)
        return remote(anchor_out.at[d], anchor_in, arecv_sem, h, to_s)

    def sends_anchor(d):
        _, to_s, _, _ = place_from(d, g)
        return also(to_s == s, jnp.logical_not(is_me(d)))

    ahead = 2 * half

    def first_rows(d, lo, size, sem):
        _, _, b0, k0 = place_from(d, g)
        return pltpu.make_async_copy(
            codes.at[b0, pl.ds(k0 + lo, size)], raw.at[0, d, pl.ds(lo, size)], sem
        )

    def first_loaded(lo, size, sem):
        these = raw.at[0, pl.ds(0, ahead), pl.ds(lo, size)]
        return pltpu.make_async_copy(these, these, sem)

    barrier = pltpu.get_barrier_semaphore()

    @pl.when(pass_on)
    def _():
        pl.semaphore_signal(
            barrier, inc=1, device_id={"seq": s, "grp": partner}, device_id_type=MESH
        )


    @pl.loop(0, seqs)
    def _(j):
        straight = jnp.logical_or(zone // half == g // half, j // per_grp == zone)
        to_g = jnp.where(straight, zone, zone_partner)

        @pl.when(jnp.logical_not(also(j == s, to_g == g)))
        def _():
            pl.semaphore_signal(
                barrier, inc=1, device_id={"seq": j, "grp": to_g}, device_id_type=MESH
            )

    gets_moved = also(g // half == zone_partner // half, lax.rem(g, half) == 0)

    @pl.when(also(gets_moved, lax.rem(s, per_grp) == 0))
    def _():
        @pl.loop(0, seqs if MOVED else 0)
        def _(j):
            @pl.when(j // per_grp != zone)
            def _():
                pl.semaphore_signal(
                    barrier, inc=1, device_id={"seq": j, "grp": zone}, device_id_type=MESH
                )

    for d in range(ahead):
        first_rows(d, 0, 1, first_sem).start()

    expected = (
        blocks // 2
        + jnp.where(via, 1 + (1 if MOVED else 0), blocks // 2 - 1)
        + jnp.where(pass_on, blocks // 2, 0)
    )

    if head_rows > 1:
        for d in range(ahead):
            first_rows(d, 1, head_rows - 1, rest_sem).start()

    for b in range(seq_rows):
        @pl.loop(ahead if b == 0 else 0, blocks)
        def _(d, b=b):
            load(d, b, load_sem.at[b, d // (2 * half)]).start()

    fetch_index = pltpu.make_async_copy(index_hbm, index_ref, load_sem.at[0, 0])
    fetch_anchor = pltpu.make_async_copy(anchor_hbm, anchor_ref, small_sem)
    fetch_index.start()
    fetch_anchor.start()

    t_out = lax.broadcasted_iota(jnp.int32, (tokens, tokens), 0)
    t_in = lax.broadcasted_iota(jnp.int32, (tokens, tokens), 1)
    same = t_out // group_len == t_in // group_len
    within = jnp.where(also(same, t_out >= t_in), 1.0, 0.0).astype(jnp.bfloat16)

    def compute(d, r, lo, size):
        x = raw[r // head_rows, d, lax.rem(r, head_rows), pl.ds(lo, size), :]
        x = x.astype(jnp.float32).astype(jnp.bfloat16)
        run = jnp.dot(within[:size, :size], x, preferred_element_type=jnp.float32)
        sums[d, r, pl.ds(lo, size), :] = run.astype(jnp.bfloat16)

    def moves(own):
        up = zone // half < own // half
        last = also(zone == grps - 1, lax.rem(own, half) == half - 1)
        return jnp.logical_or(up, lax.rem(own, half) == 0)

    def is_moved(own, e, i, lo, size):
        hit = size < tokens and e == 0 and (1 if lo else 0) in MOVED
        return also(i == 0, moves(own)) if hit else i < 0

    def send_all(i, r, lo, size):
        def compute_all():
            for side in range(2):
                for e in range(half):
                    compute((i * half + e) * 2 + side, r, lo, size)

        if size < tokens and lo == 0:
            pl.when(i > 0)(compute_all)
        else:
            compute_all()

        for e in range(half):
            d = (i * half + e) * 2
            relayed = also(via, jnp.logical_not(is_moved(g, e, i, lo, size)))

            @pl.when(relayed)
            def _(d=d):
                send_relay(d, r, lo, size).start()

            @pl.when(jnp.logical_not(relayed))
            def _(d=d):
                send_part(d, r, lo, size).start()

        for e in range(half):
            d = (i * half + e) * 2 + 1

            @pl.when(jnp.logical_not(is_me(d)))
            def _(d=d):
                send_part(d, r, lo, size).start()

    def forward_all(i, r, lo, size):
        def from_relay(e):
            d = (i * half + e) * 2
            forward(d, r, lo, size).start()

        if size == tokens:
            both = relay.at[pl.ds(i * half, half), r]
            here(both, relay_sem.at[i, r - 1]).wait_recv()
            for e in range(half):
                from_relay(e)
        else:
            for e in range(half):
                @pl.when(jnp.logical_not(is_moved(partner, e, i, lo, size)))
                def _(e=e):
                    send_relay((i * half + e) * 2, r, lo, size).wait_recv()
                    from_relay(e)

    lane = lax.broadcasted_iota(jnp.int32, (groups, rows * groups), 1)
    spread = (lax.rem(lane, groups) == lax.broadcasted_iota(jnp.int32, lane.shape, 0))
    lane = lax.broadcasted_iota(jnp.int32, (rows, rows * groups), 1)
    own_row = lane // groups == lax.broadcasted_iota(jnp.int32, lane.shape, 0)

    def send_small():
        fetch_index.wait()
        fetch_anchor.wait()

        ids = index_ref[...].astype(jnp.float32).astype(jnp.bfloat16)
        ids = ids.reshape(-1, groups)
        wide = jnp.dot(ids, spread.astype(jnp.bfloat16), preferred_element_type=jnp.float32)
        wide_ref[...] = wide.reshape(wide_ref.shape)

        @pl.loop(0, blocks)
        def _(d):
            _, _, b0, k0 = place_from(d, g)
            line = 0.0
            for b in range(seq_rows):
                these = pl.ds(b * head_rows, head_rows)
                anchor_out[d, these, :] = anchor_ref[b0 + b, pl.ds(k0, head_rows), :]
                kept = jnp.where(own_row[b * head_rows:(b + 1) * head_rows],
                                 wide_ref[b0 + b, pl.ds(k0, head_rows), :], 0.0)
                line += jnp.sum(kept, axis=0, keepdims=True)
            index_out[d] = line.astype(jnp.int32)

        @pl.loop(0, blocks)
        def _(d):
            relayed = also(lax.rem(d, 2) == 0, via)

            @pl.when(relayed)
            def _():
                hold_index(d).start()

            @pl.when(jnp.logical_not(jnp.logical_or(relayed, is_me(d))))
            def _():
                send_index(d).start()

            @pl.when(sends_anchor(d))
            def _():
                send_anchor(d).start()

    steps = (chunks + LEAD * (per_grp - 1)) * per_grp
    small_at = min(SMALL, steps - 1)
    first_loaded(0, 1, first_sem).wait()
    for d in range(ahead):
        compute(d, 0, 0, piece)
    pl.semaphore_wait(barrier, expected)

    def at_chunk(n, ready, do):
        i = lax.rem(n, per_grp)
        c = n // per_grp - LEAD * i
        for k, (lo, size) in enumerate(halves):
            @pl.when(also(ready, c == k))
            def _(lo=lo, size=size):
                do(i, 0, lo, size)

        @pl.when(also(ready, also(c >= 2, c < chunks)))
        def _():
            do(i, c - 1, 0, tokens)

    def wait_and_send(i, r, lo, size):
        if lo == 0:
            if head_rows > 1:
                @pl.when(also(i == 0, r == 1))
                def _():
                    first_loaded(1, head_rows - 1, rest_sem).wait()

            for b in range(seq_rows):
                for k in range(1 if b == 0 else 0, per_grp):
                    @pl.when(also(i == k, r == b * head_rows))
                    def _(b=b, k=k):
                        loaded(b, k).wait()
        send_all(i, r, lo, size)

    lag = jnp.where(zone // half == g // half, RELAY_LAG, LAG)

    @pl.loop(0, steps + LAG)
    def _(n):
        m = n - lag
        at_chunk(jnp.maximum(m, 0), also(also(m >= 0, m < steps), pass_on), forward_all)
        at_chunk(n, n < steps, wait_and_send)

        @pl.when(n == small_at)
        def _():
            send_small()

        @pl.when(also(pass_on, n == small_at + LAG))
        def _():
            here(index_hold, ihold_sem).wait_recv()

            @pl.loop(0, blocks // 2)
            def _(e):
                forward_index(e * 2).start()

    fetch_table = pltpu.make_async_copy(table_hbm, table_ref, load_sem.at[0, 0])
    fetch_scale = pltpu.make_async_copy(anchor_scale_hbm, anchor_scale_ref, small_sem)
    fetch_table.start()
    fetch_scale.start()

    @pl.loop(0, blocks)
    def _(d):
        @pl.when(is_me(d))
        def _():
            index_in[s] = index_out[d]
            anchor_in[...] = anchor_out[d]
            for r in range(rows):
                landed[r, pl.ds(pl.multiple_of(s * tokens, tokens), tokens), :] = sums[d, r]

    def fewer(part, size, sem):
        @pl.when(mine)
        def _():
            here(part(size - size // seqs), sem).wait_recv()

        @pl.when(jnp.logical_not(mine))
        def _():
            here(part(size), sem).wait_recv()

    @pl.when(jnp.logical_not(mine))
    def _():
        here(anchor_in, arecv_sem).wait_recv()

    fetch_table.wait()
    fetch_scale.wait()
    for r in range(rows):
        base_ref[r] = anchor_in[pl.ds(r, 1), :].astype(jnp.float32) * anchor_scale_ref[...]

    fewer(lambda size: index_in.at[pl.ds(0, size)], seqs, irecv_sem)

    @pl.loop(0, seqs)
    def _(j):
        many = rows * groups
        ids = jnp.broadcast_to(index_in[j], (levels, many))
        hot = (ids == lax.broadcasted_iota(jnp.int32, (levels, many), 0)).astype(jnp.float32)
        found = lax.dot_general(
            hot, table_ref[...], (((0,), (0,)), ((), ())),
            precision=HIGHEST, preferred_element_type=jnp.float32,
        )
        for r in range(rows):
            scales_ref[r, pl.ds(pl.multiple_of(j * groups, groups), groups), :] = (
                found[r * groups:(r + 1) * groups]
            )

    def finish(group, first, last):
        many_rows = pl.ds(first, last - first)
        fewer(lambda size: landed.at[many_rows, pl.ds(0, size)], seqs * tokens, recv_sem.at[group])

        @pl.loop(first, min(last, rows - min(KEEP, rows)))
        def _(r):
            many, step = grow(landed, scales_ref, base_ref, r)

            def put(j, base):
                at, built, base = step(j, base)
                landed[r, pl.ds(at, group_len), :] = built
                return base

            lax.fori_loop(0, many, put, base_ref[r], unroll=16)

    for group, first in enumerate(cuts[:-1]):
        finish(group, first, cuts[group + 1])

    def sent(ref):
        here(ref, recv_sem.at[0]).wait_send()

    @pl.when(mine)
    def _():
        sent(sums.at[pl.ds(0, blocks - 1)])
        sent(index_out.at[pl.ds(0, blocks - 1)])
        for _ in range(grps - 1):
            sent(anchor_out.at[0])

    @pl.when(jnp.logical_not(mine))
    def _():
        sent(sums)
        sent(index_out)

    @pl.when(pass_on)
    def _():
        sent(index_hold)
        if MOVED:
            sent(relay.at[pl.ds(1, blocks // 2 - 1)])
            if rows > 1:
                sent(relay.at[0, pl.ds(1, rows - 1)])
            for lo, size in halves:
                @pl.when(jnp.logical_not(is_moved(partner, 0, 0, lo, size)))
                def _(lo=lo, size=size):
                    sent(relay.at[0, 0, pl.ds(lo, size)])
        else:
            sent(relay)


def rebuild(landed, scales_ref, base_ref, out_hbm, built, out_sem):
    rows = landed.shape[0]
    keep = built.shape[0]
    done = rows - keep
    stores = []
    if done:
        these = pl.ds(0, done)
        stores.append(pltpu.make_async_copy(landed.at[these], out_hbm.at[0, these], out_sem.at[keep]))
        stores[0].start()
    for q in range(keep):
        r = done + q
        many, step = grow(landed, scales_ref, base_ref, r)
        group_len = landed.shape[1] // many

        def put(j, base, q=q, step=step):
            at, grown, base = step(j, base)
            built[q, pl.ds(at, group_len), :] = grown
            return base

        lax.fori_loop(0, many, put, base_ref[r], unroll=16)
        stores.append(pltpu.make_async_copy(built.at[q], out_hbm.at[0, r], out_sem.at[q]))
        stores[-1].start()
    for store in stores:
        store.wait()


def on_device(delta_codes, scale_index, anchor_codes, scale_table, anchor_scale):
    seqs, grps = lax.axis_size("seq"), lax.axis_size("grp")
    seq_local, kv_heads, tokens, channels = delta_codes.shape
    groups = scale_index.shape[2]
    heads = kv_heads // grps
    rows = seq_local * grps * heads // seqs
    blocks = seq_local * kv_heads // rows
    seq_rows, head_rows = max(1, rows // heads), min(rows, heads)
    keep = min(KEEP, rows)
    length = seqs * tokens
    vmem = pl.BlockSpec(memory_space=pltpu.VMEM)
    hbm = pl.BlockSpec(memory_space=pltpu.HBM)
    operands = (delta_codes, scale_index, anchor_codes, scale_table, anchor_scale[None])
    landed, scales, base = pl.pallas_call(
        exchange,
        out_shape=(
            jax.ShapeDtypeStruct((rows, length, channels), jnp.bfloat16),
            jax.ShapeDtypeStruct((rows, seqs * groups, channels), jnp.float32),
            jax.ShapeDtypeStruct((rows, 1, channels), jnp.float32),
        ),
        in_specs=[hbm] * 5,
        out_specs=(vmem, vmem, vmem),
        scratch_shapes=[
            pltpu.VMEM((seq_rows, blocks, head_rows, tokens, channels), jnp.int32),
            pltpu.VMEM((blocks, rows, tokens, channels), jnp.bfloat16),
            pltpu.VMEM((blocks // 2, rows, tokens, channels), jnp.bfloat16),
            pltpu.VMEM((blocks, 1, rows * groups), jnp.int32),
            pltpu.VMEM((blocks // 2, 1, rows * groups), jnp.int32),
            pltpu.VMEM((seqs, 1, rows * groups), jnp.int32),
            pltpu.VMEM((blocks, rows, channels), jnp.int32),
            pltpu.VMEM((rows, channels), jnp.int32),
            pltpu.SemaphoreType.DMA,
            pltpu.SemaphoreType.DMA,
            pltpu.SemaphoreType.DMA((seq_rows, blocks // grps)),
            pltpu.SemaphoreType.DMA,
            pltpu.SemaphoreType.DMA((len(arrival_cuts(rows)) - 1,)),
            pltpu.SemaphoreType.DMA,
            pltpu.SemaphoreType.DMA,
            pltpu.SemaphoreType.DMA,
            pltpu.SemaphoreType.DMA((blocks // 2, 2)),
            pltpu.SemaphoreType.DMA((blocks // grps, max(1, rows - 1))),
            pltpu.VMEM(scale_index.shape, jnp.int32),
            pltpu.VMEM(anchor_codes.shape, jnp.int32),
            pltpu.VMEM(scale_table.shape, jnp.float32),
            pltpu.VMEM((1, channels), jnp.float32),
            pltpu.SemaphoreType.DMA,
            pltpu.VMEM(scale_index.shape[:2] + (rows * groups,), jnp.float32),
        ],
        compiler_params=pltpu.CompilerParams(
            collective_id=0, has_side_effects=True, vmem_limit_bytes=48 * 1024 * 1024
        ),
        name="exchange",
    )(*(pltpu.with_memory_space_constraint(x, pltpu.HBM) for x in operands))

    return pl.pallas_call(
        rebuild,
        out_shape=jax.ShapeDtypeStruct((1, rows, length, channels), jnp.bfloat16),
        in_specs=[vmem] * 3,
        out_specs=hbm,
        scratch_shapes=[
            pltpu.VMEM((keep, length, channels), jnp.bfloat16),
            pltpu.SemaphoreType.DMA((keep + 1,)),
        ],
        compiler_params=pltpu.CompilerParams(vmem_limit_bytes=16 * 1024 * 1024),
        name="rebuild",
    )(landed, scales, base)


def solution(mesh):
    placed = (P("grp", None, "seq", None), P("grp", None, "seq"), P("grp", None, None), P(), P())
    return jax.shard_map(
        on_device,
        mesh=mesh,
        in_specs=placed,
        out_specs=P("grp", "seq", None, None),
        check_vma=False,
    )
```

```python
import jax
import jax.numpy as jnp
from jax import lax
from jax.experimental import pallas as pl
from jax.experimental.pallas import tpu as pltpu
from jax.sharding import PartitionSpec as P

MESH = pl.DeviceIdType.MESH
MOVED = (1,)
SMALL = 6
LEAD = 0
LAG = 4
FIRST = 2
RELAY_LAG = 1
KEEP = 1
HIGHEST = lax.Precision.HIGHEST


def grow(landed, scales_ref, base_ref, r):
    groups = scales_ref.shape[1]
    group_len = landed.shape[1] // groups

    def step(j, base):
        at = pl.multiple_of(j * group_len, group_len)
        x = landed[r, pl.ds(at, group_len), :].astype(jnp.float32)
        grown = x * scales_ref[r, pl.ds(j, 1), :]
        return at, (grown + base).astype(jnp.bfloat16), base + grown[group_len - 1:]

    return groups, step


def arrival_cuts(rows):
    return sorted({0, rows // 2, rows - min(KEEP, rows), rows})


def exchange(
    codes, index_hbm, anchor_hbm, table_hbm, anchor_scale_hbm,
    landed, scales_ref, base_ref,
    raw, sums, relay, index_out, index_hold, index_in, anchor_out, anchor_in,
    first_sem, rest_sem, load_sem, send_sem, recv_sem, ihold_sem, irecv_sem, arecv_sem,
    relay_half_sem, relay_sem,
    index_ref, anchor_ref, table_ref, anchor_scale_ref, small_sem, wide_ref,
):
    seqs, grps = lax.axis_size("seq"), lax.axis_size("grp")
    s, g = lax.axis_index("seq"), lax.axis_index("grp")
    blocks, rows, tokens, channels = sums.shape
    heads = codes.shape[1] // grps
    per_grp = blocks // grps
    half = grps // 2
    partner = lax.rem(g + half, grps)
    seq_rows, head_rows = raw.shape[0], raw.shape[2]
    levels = table_ref.shape[0]
    groups = index_hbm.shape[2]
    group_len = tokens // groups
    piece = tokens // FIRST
    halves = ((0, piece), (piece, tokens - piece))
    zone = s // per_grp
    zone_partner = lax.rem(zone + half, grps)
    via = zone != g
    pass_on = zone != partner
    mine = zone == g
    also = jnp.logical_and
    chunks = rows + 1
    cuts = arrival_cuts(rows)

    def arrival_sem(r):
        group = 0
        for at in cuts[1:-1]:
            group = group + jnp.where(r >= at, 1, 0)
        return recv_sem.at[group]


    def place_from(d, own):
        side, e, i = lax.rem(d, 2), lax.rem(d // 2, half), d // 2 // half
        h = lax.rem(own // half + 1 + side, 2) * half + lax.rem(e + i, half)
        first = i * rows
        return h, own * per_grp + i, first // heads, h * heads + lax.rem(first, heads)

    def is_me(d):
        h, to_s, _, _ = place_from(d, g)
        return also(h == g, to_s == s)

    def load(d, b, sem):
        _, _, b0, k0 = place_from(d, g)
        return pltpu.make_async_copy(codes.at[b0 + b, pl.ds(k0, head_rows)], raw.at[b, d], sem)

    def loaded(b, i):
        these = raw.at[b, pl.ds(i * 2 * half, 2 * half)]
        return pltpu.make_async_copy(these, these, load_sem.at[b, i])

    def spot(r, lo, size):
        return landed.at[r, pl.ds(pl.multiple_of(s * tokens + lo, piece), size), :]

    def remote(src, dst, rsem, h, to_s):
        return pltpu.make_async_remote_copy(
            src_ref=src, dst_ref=dst, send_sem=send_sem, recv_sem=rsem,
            device_id={"seq": to_s, "grp": h}, device_id_type=MESH,
        )

    def here(ref, rsem):
        return remote(ref, ref, rsem, g, s)

    def relay_sem_at(d, r, lo, size):
        if size == tokens:
            return relay_sem.at[d // 2 // half, r - 1]
        return relay_half_sem.at[d // 2, 1 if lo else 0]

    def send_relay(d, r, lo, size):
        return remote(
            sums.at[d, r, pl.ds(lo, size)], relay.at[d // 2, r, pl.ds(lo, size)],
            relay_sem_at(d, r, lo, size), partner, s,
        )

    def send_part(d, r, lo, size):
        h, to_s, _, _ = place_from(d, g)
        return remote(sums.at[d, r, pl.ds(lo, size)], spot(r, lo, size), arrival_sem(r), h, to_s)

    def forward(d, r, lo, size):
        h, to_s, _, _ = place_from(d, partner)
        return remote(
            relay.at[d // 2, r, pl.ds(lo, size)], spot(r, lo, size), arrival_sem(r), h, to_s
        )

    def send_index(d):
        h, to_s, _, _ = place_from(d, g)
        return remote(index_out.at[d], index_in.at[s], irecv_sem, h, to_s)

    def hold_index(d):
        return remote(index_out.at[d], index_hold.at[d // 2], ihold_sem, partner, s)

    def forward_index(d):
        h, to_s, _, _ = place_from(d, partner)
        return remote(index_hold.at[d // 2], index_in.at[s], irecv_sem, h, to_s)

    def send_anchor(d):
        h, to_s, _, _ = place_from(d, g)
        return remote(anchor_out.at[d], anchor_in, arecv_sem, h, to_s)

    def sends_anchor(d):
        _, to_s, _, _ = place_from(d, g)
        return also(to_s == s, jnp.logical_not(is_me(d)))

    ahead = 2 * half

    def first_rows(d, lo, size, sem):
        _, _, b0, k0 = place_from(d, g)
        return pltpu.make_async_copy(
            codes.at[b0, pl.ds(k0 + lo, size)], raw.at[0, d, pl.ds(lo, size)], sem
        )

    def first_loaded(lo, size, sem):
        these = raw.at[0, pl.ds(0, ahead), pl.ds(lo, size)]
        return pltpu.make_async_copy(these, these, sem)

    barrier = pltpu.get_barrier_semaphore()

    @pl.when(pass_on)
    def _():
        pl.semaphore_signal(
            barrier, inc=1, device_id={"seq": s, "grp": partner}, device_id_type=MESH
        )


    @pl.loop(0, seqs)
    def _(j):
        straight = jnp.logical_or(zone // half == g // half, j // per_grp == zone)
        to_g = jnp.where(straight, zone, zone_partner)

        @pl.when(jnp.logical_not(also(j == s, to_g == g)))
        def _():
            pl.semaphore_signal(
                barrier, inc=1, device_id={"seq": j, "grp": to_g}, device_id_type=MESH
            )

    gets_moved = also(g // half == zone_partner // half, lax.rem(g, half) == 0)

    @pl.when(also(gets_moved, lax.rem(s, per_grp) == 0))
    def _():
        @pl.loop(0, seqs if MOVED else 0)
        def _(j):
            @pl.when(j // per_grp != zone)
            def _():
                pl.semaphore_signal(
                    barrier, inc=1, device_id={"seq": j, "grp": zone}, device_id_type=MESH
                )

    for d in range(ahead):
        first_rows(d, 0, 1, first_sem).start()

    expected = (
        blocks // 2
        + jnp.where(via, 1 + (1 if MOVED else 0), blocks // 2 - 1)
        + jnp.where(pass_on, blocks // 2, 0)
    )

    if head_rows > 1:
        for d in range(ahead):
            first_rows(d, 1, head_rows - 1, rest_sem).start()

    def load_all(b, first):
        @pl.loop(first, blocks)
        def _(d):
            load(d, b, load_sem.at[b, d // (2 * half)]).start()

    load_all(0, ahead)
    fetch_index = pltpu.make_async_copy(index_hbm, index_ref, small_sem.at[0])
    fetch_anchor = pltpu.make_async_copy(anchor_hbm, anchor_ref, small_sem.at[1])
    fetch_index.start()
    fetch_anchor.start()

    t_out = lax.broadcasted_iota(jnp.int32, (tokens, tokens), 0)
    t_in = lax.broadcasted_iota(jnp.int32, (tokens, tokens), 1)
    same = t_out // group_len == t_in // group_len
    within = jnp.where(also(same, t_out >= t_in), 1.0, 0.0).astype(jnp.bfloat16)

    def compute(d, r, lo, size):
        x = raw[r // head_rows, d, lax.rem(r, head_rows), pl.ds(lo, size), :]
        x = x.astype(jnp.float32).astype(jnp.bfloat16)
        run = jnp.dot(within[:size, :size], x, preferred_element_type=jnp.float32)
        sums[d, r, pl.ds(lo, size), :] = run.astype(jnp.bfloat16)

    def moves(own):
        up = zone // half < own // half
        last = also(zone == grps - 1, lax.rem(own, half) == half - 1)
        return jnp.logical_or(up, lax.rem(own, half) == 0)

    def is_moved(own, e, i, lo, size):
        hit = size < tokens and e == 0 and (1 if lo else 0) in MOVED
        return also(i == 0, moves(own)) if hit else i < 0

    def send_all(i, r, lo, size):
        def compute_all():
            for side in range(2):
                for e in range(half):
                    compute((i * half + e) * 2 + side, r, lo, size)

        if size < tokens and lo == 0:
            pl.when(i > 0)(compute_all)
        else:
            compute_all()

        for e in range(half):
            d = (i * half + e) * 2
            relayed = also(via, jnp.logical_not(is_moved(g, e, i, lo, size)))

            @pl.when(relayed)
            def _(d=d):
                send_relay(d, r, lo, size).start()

            @pl.when(jnp.logical_not(relayed))
            def _(d=d):
                send_part(d, r, lo, size).start()

        for e in range(half):
            d = (i * half + e) * 2 + 1

            @pl.when(jnp.logical_not(is_me(d)))
            def _(d=d):
                send_part(d, r, lo, size).start()

    def forward_all(i, r, lo, size):
        def from_relay(e):
            d = (i * half + e) * 2
            forward(d, r, lo, size).start()

        if size == tokens:
            both = relay.at[pl.ds(i * half, half), r]
            here(both, relay_sem.at[i, r - 1]).wait_recv()
            for e in range(half):
                from_relay(e)
        else:
            for e in range(half):
                @pl.when(jnp.logical_not(is_moved(partner, e, i, lo, size)))
                def _(e=e):
                    send_relay((i * half + e) * 2, r, lo, size).wait_recv()
                    from_relay(e)

    lane = lax.broadcasted_iota(jnp.int32, (groups, rows * groups), 1)
    spread = (lax.rem(lane, groups) == lax.broadcasted_iota(jnp.int32, lane.shape, 0))
    lane = lax.broadcasted_iota(jnp.int32, (rows, rows * groups), 1)
    own_row = lane // groups == lax.broadcasted_iota(jnp.int32, lane.shape, 0)

    def send_small():
        fetch_index.wait()
        fetch_anchor.wait()

        ids = index_ref[...].astype(jnp.float32).astype(jnp.bfloat16)
        ids = ids.reshape(-1, groups)
        wide = jnp.dot(ids, spread.astype(jnp.bfloat16), preferred_element_type=jnp.float32)
        wide_ref[...] = wide.reshape(wide_ref.shape)

        @pl.loop(0, blocks)
        def _(d):
            _, _, b0, k0 = place_from(d, g)
            line = 0.0
            for b in range(seq_rows):
                these = pl.ds(b * head_rows, head_rows)
                anchor_out[d, these, :] = anchor_ref[b0 + b, pl.ds(k0, head_rows), :]
                kept = jnp.where(own_row[b * head_rows:(b + 1) * head_rows],
                                 wide_ref[b0 + b, pl.ds(k0, head_rows), :], 0.0)
                line += jnp.sum(kept, axis=0, keepdims=True)
            index_out[d] = line.astype(jnp.int32)

        @pl.loop(0, blocks)
        def _(d):
            relayed = also(lax.rem(d, 2) == 0, via)

            @pl.when(relayed)
            def _():
                hold_index(d).start()

            @pl.when(jnp.logical_not(jnp.logical_or(relayed, is_me(d))))
            def _():
                send_index(d).start()

            @pl.when(sends_anchor(d))
            def _():
                send_anchor(d).start()

    steps = (chunks + LEAD * (per_grp - 1)) * per_grp
    small_at = min(SMALL, steps - 1)
    first_loaded(0, 1, first_sem).wait()
    for d in range(ahead):
        compute(d, 0, 0, piece)
    pl.semaphore_wait(barrier, expected)
    for b in range(1, seq_rows):
        load_all(b, 0)

    def at_chunk(n, ready, do):
        i = lax.rem(n, per_grp)
        c = n // per_grp - LEAD * i
        for k, (lo, size) in enumerate(halves):
            @pl.when(also(ready, c == k))
            def _(lo=lo, size=size):
                do(i, 0, lo, size)

        @pl.when(also(ready, also(c >= 2, c < chunks)))
        def _():
            do(i, c - 1, 0, tokens)

    def wait_and_send(i, r, lo, size):
        if lo == 0:
            if head_rows > 1:
                @pl.when(also(i == 0, r == 1))
                def _():
                    first_loaded(1, head_rows - 1, rest_sem).wait()

            for b in range(seq_rows):
                for k in range(1 if b == 0 else 0, per_grp):
                    @pl.when(also(i == k, r == b * head_rows))
                    def _(b=b, k=k):
                        loaded(b, k).wait()
        send_all(i, r, lo, size)

    lag = jnp.where(zone // half == g // half, RELAY_LAG, LAG)

    @pl.loop(0, steps + LAG)
    def _(n):
        m = n - lag
        at_chunk(jnp.maximum(m, 0), also(also(m >= 0, m < steps), pass_on), forward_all)
        at_chunk(n, n < steps, wait_and_send)

        @pl.when(n == small_at)
        def _():
            send_small()

        @pl.when(also(pass_on, n == small_at + LAG))
        def _():
            here(index_hold, ihold_sem).wait_recv()

            @pl.loop(0, blocks // 2)
            def _(e):
                forward_index(e * 2).start()

    fetch_table = pltpu.make_async_copy(table_hbm, table_ref, small_sem.at[0])
    fetch_scale = pltpu.make_async_copy(anchor_scale_hbm, anchor_scale_ref, small_sem.at[1])
    fetch_table.start()
    fetch_scale.start()

    @pl.loop(0, blocks)
    def _(d):
        @pl.when(is_me(d))
        def _():
            index_in[s] = index_out[d]
            anchor_in[...] = anchor_out[d]
            for r in range(rows):
                landed[r, pl.ds(pl.multiple_of(s * tokens, tokens), tokens), :] = sums[d, r]

    def fewer(part, size, sem):
        @pl.when(mine)
        def _():
            here(part(size - size // seqs), sem).wait_recv()

        @pl.when(jnp.logical_not(mine))
        def _():
            here(part(size), sem).wait_recv()

    @pl.when(jnp.logical_not(mine))
    def _():
        here(anchor_in, arecv_sem).wait_recv()

    fetch_table.wait()
    fetch_scale.wait()
    for r in range(rows):
        base_ref[r] = anchor_in[pl.ds(r, 1), :].astype(jnp.float32) * anchor_scale_ref[...]

    fewer(lambda size: index_in.at[pl.ds(0, size)], seqs, irecv_sem)

    @pl.loop(0, seqs)
    def _(j):
        many = rows * groups
        ids = jnp.broadcast_to(index_in[j], (levels, many))
        hot = (ids == lax.broadcasted_iota(jnp.int32, (levels, many), 0)).astype(jnp.float32)
        found = lax.dot_general(
            hot, table_ref[...], (((0,), (0,)), ((), ())),
            precision=HIGHEST, preferred_element_type=jnp.float32,
        )
        for r in range(rows):
            scales_ref[r, pl.ds(pl.multiple_of(j * groups, groups), groups), :] = (
                found[r * groups:(r + 1) * groups]
            )

    def finish(group, first, last):
        many_rows = pl.ds(first, last - first)
        fewer(lambda size: landed.at[many_rows, pl.ds(0, size)], seqs * tokens, recv_sem.at[group])

        @pl.loop(first, min(last, rows - min(KEEP, rows)))
        def _(r):
            many, step = grow(landed, scales_ref, base_ref, r)

            def put(j, base):
                at, built, base = step(j, base)
                landed[r, pl.ds(at, group_len), :] = built
                return base

            lax.fori_loop(0, many, put, base_ref[r], unroll=16)

    for group, first in enumerate(cuts[:-1]):
        finish(group, first, cuts[group + 1])

    def sent(ref):
        here(ref, recv_sem.at[0]).wait_send()

    @pl.when(mine)
    def _():
        sent(sums.at[pl.ds(0, blocks - 1)])
        sent(index_out.at[pl.ds(0, blocks - 1)])
        for _ in range(grps - 1):
            sent(anchor_out.at[0])

    @pl.when(jnp.logical_not(mine))
    def _():
        sent(sums)
        sent(index_out)

    @pl.when(pass_on)
    def _():
        sent(index_hold)
        if MOVED:
            sent(relay.at[pl.ds(1, blocks // 2 - 1)])
            if rows > 1:
                sent(relay.at[0, pl.ds(1, rows - 1)])
            for lo, size in halves:
                @pl.when(jnp.logical_not(is_moved(partner, 0, 0, lo, size)))
                def _(lo=lo, size=size):
                    sent(relay.at[0, 0, pl.ds(lo, size)])
        else:
            sent(relay)


def rebuild(landed, scales_ref, base_ref, out_hbm, built, out_sem):
    rows = landed.shape[0]
    keep = built.shape[0]
    done = rows - keep
    stores = []
    if done:
        these = pl.ds(0, done)
        stores.append(pltpu.make_async_copy(landed.at[these], out_hbm.at[0, these], out_sem.at[keep]))
        stores[0].start()
    for q in range(keep):
        r = done + q
        many, step = grow(landed, scales_ref, base_ref, r)
        group_len = landed.shape[1] // many

        def put(j, base, q=q, step=step):
            at, grown, base = step(j, base)
            built[q, pl.ds(at, group_len), :] = grown
            return base

        lax.fori_loop(0, many, put, base_ref[r], unroll=16)
        stores.append(pltpu.make_async_copy(built.at[q], out_hbm.at[0, r], out_sem.at[q]))
        stores[-1].start()
    for store in stores:
        store.wait()


def on_device(delta_codes, scale_index, anchor_codes, scale_table, anchor_scale):
    seqs, grps = lax.axis_size("seq"), lax.axis_size("grp")
    seq_local, kv_heads, tokens, channels = delta_codes.shape
    groups = scale_index.shape[2]
    heads = kv_heads // grps
    rows = seq_local * grps * heads // seqs
    blocks = seq_local * kv_heads // rows
    seq_rows, head_rows = max(1, rows // heads), min(rows, heads)
    keep = min(KEEP, rows)
    length = seqs * tokens
    vmem = pl.BlockSpec(memory_space=pltpu.VMEM)
    hbm = pl.BlockSpec(memory_space=pltpu.HBM)
    operands = (delta_codes, scale_index, anchor_codes, scale_table, anchor_scale[None])
    landed, scales, base = pl.pallas_call(
        exchange,
        out_shape=(
            jax.ShapeDtypeStruct((rows, length, channels), jnp.bfloat16),
            jax.ShapeDtypeStruct((rows, seqs * groups, channels), jnp.float32),
            jax.ShapeDtypeStruct((rows, 1, channels), jnp.float32),
        ),
        in_specs=[hbm] * 5,
        out_specs=(vmem, vmem, vmem),
        scratch_shapes=[
            pltpu.VMEM((seq_rows, blocks, head_rows, tokens, channels), jnp.int32),
            pltpu.VMEM((blocks, rows, tokens, channels), jnp.bfloat16),
            pltpu.VMEM((blocks // 2, rows, tokens, channels), jnp.bfloat16),
            pltpu.VMEM((blocks, 1, rows * groups), jnp.int32),
            pltpu.VMEM((blocks // 2, 1, rows * groups), jnp.int32),
            pltpu.VMEM((seqs, 1, rows * groups), jnp.int32),
            pltpu.VMEM((blocks, rows, channels), jnp.int32),
            pltpu.VMEM((rows, channels), jnp.int32),
            pltpu.SemaphoreType.DMA,
            pltpu.SemaphoreType.DMA,
            pltpu.SemaphoreType.DMA((seq_rows, blocks // grps)),
            pltpu.SemaphoreType.DMA,
            pltpu.SemaphoreType.DMA((len(arrival_cuts(rows)) - 1,)),
            pltpu.SemaphoreType.DMA,
            pltpu.SemaphoreType.DMA,
            pltpu.SemaphoreType.DMA,
            pltpu.SemaphoreType.DMA((blocks // 2, 2)),
            pltpu.SemaphoreType.DMA((blocks // grps, max(1, rows - 1))),
            pltpu.VMEM(scale_index.shape, jnp.int32),
            pltpu.VMEM(anchor_codes.shape, jnp.int32),
            pltpu.VMEM(scale_table.shape, jnp.float32),
            pltpu.VMEM((1, channels), jnp.float32),
            pltpu.SemaphoreType.DMA((2,)),
            pltpu.VMEM(scale_index.shape[:2] + (rows * groups,), jnp.float32),
        ],
        compiler_params=pltpu.CompilerParams(
            collective_id=0, has_side_effects=True, vmem_limit_bytes=48 * 1024 * 1024
        ),
        name="exchange",
    )(*(pltpu.with_memory_space_constraint(x, pltpu.HBM) for x in operands))

    return pl.pallas_call(
        rebuild,
        out_shape=jax.ShapeDtypeStruct((1, rows, length, channels), jnp.bfloat16),
        in_specs=[vmem] * 3,
        out_specs=hbm,
        scratch_shapes=[
            pltpu.VMEM((keep, length, channels), jnp.bfloat16),
            pltpu.SemaphoreType.DMA((keep + 1,)),
        ],
        compiler_params=pltpu.CompilerParams(vmem_limit_bytes=16 * 1024 * 1024),
        name="rebuild",
    )(landed, scales, base)


def solution(mesh):
    placed = (P("grp", None, "seq", None), P("grp", None, "seq"), P("grp", None, None), P(), P())
    return jax.shard_map(
        on_device,
        mesh=mesh,
        in_specs=placed,
        out_specs=P("grp", "seq", None, None),
        check_vma=False,
    )
```
